32 devices in a mesh: seq: 16 (over z, y, x), rep: 2 (over core).
Axes of the slice: x: 2, y: 2, z: 4, core: 2. Of those that a mesh axis runs over, the one named last changes fastest.
Arguments:
- queries: bfloat16 [4096, 4096], P(('rep', 'seq')), parts along dimension 0, may hold values from -160 to 160
- keys_values: bfloat16 [2, 4096, 1024], P(None, ('rep', 'seq')), parts along dimension 1, may hold values from -6 to 6
- segment_ids: int32 [4096], P(('rep', 'seq')), parts along dimension 0, may hold values from 0 to 31, never falling along the last dimension, each value on 1 to 1024 neighbouring positions
Outputs:
- attended: bfloat16 [4096, 4096], P(('rep', 'seq')), parts along dimension 0
The draws below stay inside these ranges and needn't reach their ends.
There are 2 independent parts, one for each index of `rep`. The reference program is written for one: setup_inputs(seed, part) draws one part's arguments, and reference() takes and returns one part's arrays. A program takes and returns all parts, laid end to end along the dimension named above; each array names one. Nothing has to cross between parts.
Inputs may be any that keep to these rules, and one draw needn't show every extreme that they name: `segment_ids`: ids never fall along the tokens; every document holds 1 to 1024 consecutive tokens, one exactly 1024.
All inputs are finite; a program needn't handle non-finite values.
Results may differ from the reference program's by a relative error of at most 0.004.
Values may be sent and summed in bfloat16 or wider, within the bound.
A program may use at most 192 MiB of HBM per device.

```python
import math
import jax
import jax.numpy as jnp
import numpy as np
from jax import lax

HQ = 32
HK = 8
DH = 128
WINDOW = 2048
DOC_COUNT = 32
TOKENS = 2048
DOC_MOST = 1024


def shared_draw(key):
    shape_keys = (TOKENS, HK * DH)
    key_rows = jnp.clip(jax.random.normal(jax.random.fold_in(key, 101), shape_keys, jnp.float32), -6.0, 6.0)
    value_rows = jnp.clip(jax.random.normal(jax.random.fold_in(key, 102), shape_keys, jnp.float32), -6.0, 6.0)
    query_rows = jnp.clip(jax.random.normal(jax.random.fold_in(key, 103), (TOKENS, HQ * DH), jnp.float32), -6.0, 6.0)
    return (query_rows, jnp.stack([key_rows, value_rows]))


def draw_queries(key, part):
    return shared_draw(key)[0].astype(jnp.bfloat16)


def draw_keys_values(key, part):
    return shared_draw(key)[1].astype(jnp.bfloat16)


def length_profile(amount, total, limit, slope):
    weights = [(1 << 20) // math.isqrt(standing ** slope) + 1 for standing in range(2, amount + 1)]
    spare, given = total - limit - (amount - 1), [1] * (amount - 1)
    while spare > 0:
        free = [i for i in range(amount - 1) if given[i] < limit]
        whole, budget = sum([weights[i] for i in free]), spare
        for i in free:
            addition = min(limit - given[i], max(1, budget * weights[i] // whole), spare)
            given[i] = given[i] + addition
            spare = spare - addition
    return np.array([limit] + given)


def uneven_parts(own_key, number_of, total, limit, skew):
    if number_of == 2:
        one = jax.random.randint(own_key, (), max(1, total - limit), min(limit, total - 1) + 1)
        return jnp.stack([one, total - one])
    tallies = jnp.asarray(length_profile(number_of, total, limit, skew), jnp.int32)
    couples = (number_of - 1) // 2
    donor, receiver = tallies[1:1 + 2 * couples:2], tallies[2:2 + 2 * couples:2]
    room = jnp.minimum(donor - 1, limit - receiver)
    moved = jax.random.randint(jax.random.fold_in(own_key, 1), (couples,), 0, 1 << 20) % (room + 1)
    tallies = tallies.at[1:1 + 2 * couples:2].set(donor - moved).at[2:2 + 2 * couples:2].set(receiver + moved)
    return tallies[jax.random.permutation(jax.random.fold_in(own_key, 2), number_of)]


def setup_inputs(seed: int = 0, part: int = 0) -> dict:
    streams_of = jax.random.split(jax.random.key(seed), 4)
    part_keys = jax.random.split(jax.random.fold_in(streams_of[3], part), 4)
    queries = draw_queries(jax.random.fold_in(jax.random.fold_in(streams_of[3], part), 71), part)
    keys_values = draw_keys_values(jax.random.fold_in(jax.random.fold_in(streams_of[3], part), 71), part)
    segment_ids = jnp.searchsorted(jnp.cumsum(uneven_parts(part_keys[2], DOC_COUNT, TOKENS, DOC_MOST, 2)), jnp.arange(TOKENS), side="right").astype(jnp.int32)
    return dict(queries=queries, keys_values=keys_values, segment_ids=segment_ids)


def reference(queries, keys_values, segment_ids):
    group_size = HQ // HK
    score_scale = DH ** -0.5
    query_rows = min(512, TOKENS)
    key_span = WINDOW + query_rows
    key_table = jnp.pad(keys_values[0], ((WINDOW, 0), (0, 0)))
    value_table = jnp.pad(keys_values[1], ((WINDOW, 0), (0, 0)))
    padded_ids = jnp.pad(segment_ids, (WINDOW, 0), constant_values=-1)

    def one_block(number):
        first_row = (number * query_rows).astype(jnp.int32)
        query_block = lax.dynamic_slice_in_dim(queries, first_row, query_rows, 0)
        query_block = query_block.reshape(query_rows, HK, group_size, DH).astype(jnp.float32)
        key_block = lax.dynamic_slice_in_dim(key_table, first_row, key_span, 0).reshape(key_span, HK, DH).astype(jnp.float32)
        value_block = lax.dynamic_slice_in_dim(value_table, first_row, key_span, 0).reshape(key_span, HK, DH).astype(jnp.float32)
        query_ids = lax.dynamic_slice_in_dim(segment_ids, first_row, query_rows, 0)
        key_ids = lax.dynamic_slice_in_dim(padded_ids, first_row, key_span, 0)
        query_place = jnp.arange(query_rows, dtype=jnp.int32) + WINDOW
        key_place = jnp.arange(key_span, dtype=jnp.int32)
        distance = query_place[:, None] - key_place[None, :]
        allowed = (query_ids[:, None] == key_ids[None, :]) & (distance >= 0) & (distance < WINDOW)
        scores = jnp.einsum("qhgd,khd->hgqk", query_block, key_block) * score_scale
        scores = jnp.where(allowed, scores, -1.0e30)
        top = jnp.max(scores, axis=-1, keepdims=True)
        weights = jnp.where(allowed, jnp.exp(scores - top), 0.0)
        totals = jnp.sum(weights, axis=-1)
        rounded = lax.optimization_barrier(weights.astype(jnp.bfloat16))
        context = jnp.einsum("hgqk,khd->hgqd", rounded.astype(jnp.float32), value_block)
        result = context / totals[..., None]
        return jnp.transpose(result, (2, 0, 1, 3)).reshape(query_rows, HQ * DH).astype(jnp.bfloat16)

    blocks = lax.map(one_block, jnp.arange(TOKENS // query_rows, dtype=jnp.int32))
    return blocks.reshape(TOKENS, HQ * DH)
```

```python
import functools
import math

import jax
import jax.numpy as jnp
from jax import lax
from jax.experimental import pallas as pl
from jax.experimental.pallas import tpu as pltpu
from jax.sharding import PartitionSpec as P

HQ = 32
HK = 8
DH = 128
WINDOW = 2048
GROUP = HQ // HK
WIDE = GROUP * DH
SPAN = 4
SERVED = 4
NEG_BIG = -1e30
SCALE2 = DH ** (-0.5) * math.log2(math.e)
IDS = HK
PIECES = [IDS] + list(range(HK))


def kernel(n, rows, back, q_hbm, kv_hbm, ids_hbm, out_hbm, buf, ids_buf, q_buf, q_up, ids_up, out_buf, part_out, part_in,
           lse_out, lse_in, bias, bias_up, run_max, run_sum, run_acc, in_sem, out_sem, send_sem, recv_sem, down_send,
           down_recv, part_send, part_recv):
    top_level = back // SPAN
    planes = n // SPAN
    group_rows = GROUP * rows
    me = lax.axis_index("seq")
    plane = me // SPAN
    spot = me % SPAN
    low, high = spot % 2, spot // 2
    spot_x = (1 - low) + 2 * high
    spot_y = low + 2 * (1 - high)
    spot_d = (1 - low) + 2 * (1 - high)
    spots = (spot, spot_x, spot_y, spot_d)
    dev_x = plane * SPAN + spot_x
    dev_y = plane * SPAN + spot_y
    up_ok = plane < planes - 1
    down_ok = plane > 0
    dev_up = jnp.where(up_ok, me + SPAN, me - SPAN)
    dev_down = jnp.where(down_ok, me - SPAN, me + SPAN)

    def last_of(c):
        return top_level - 1 if c < SERVED else top_level

    def later(block, t):
        return (block > t).astype(jnp.int32)

    def need(s, t, block, c):
        gap = SPAN * s + t - block
        return (plane >= s) & (gap >= 1) & (gap <= SPAN * last_of(c))

    def ends_in_x(s, t, c):
        mixed = (t % 2) != (t // 2)
        edge = s == 0 or s == last_of(c)
        if edge:
            return mixed | (c % 2 == 0)
        return jnp.logical_not(mixed) & (c % 2 == 0)

    def ref_of(level, r, c):
        if c == IDS:
            return ids_buf.at[level, r]
        return buf.at[level, c, :, r]

    def copy(s, r, c, lane, to_s, to_r, device, to_spot):
        level, to_level = s - later(spots[r], spot), to_s - later(spots[r], to_spot)
        return pltpu.make_async_remote_copy(
            src_ref=ref_of(level, r, c),
            dst_ref=ref_of(to_level, to_r, c),
            send_sem=send_sem.at[s, lane, c],
            recv_sem=recv_sem.at[to_level, to_r, c],
            device_id={"seq": device},
            device_id_type=pl.DeviceIdType.MESH,
        )

    def wait_slot(level, r, c):
        pltpu.make_async_remote_copy(
            src_ref=ref_of(level, r, c),
            dst_ref=ref_of(level, r, c),
            send_sem=send_sem.at[0, 0, c],
            recv_sem=recv_sem.at[level, r, c],
            device_id={"seq": dev_x},
            device_id_type=pl.DeviceIdType.MESH,
        ).wait_recv()

    def up_copy(s, c):
        return up_ok & (plane >= s), copy(s, 0, c, 2, s + 1, 0, dev_up, spot)

    def x_copy(s, c):
        return need(s, spot_x, spot, c), copy(s, 0, c, 0, s, 1, dev_x, spot_x)

    def y_copy(s, c):
        return need(s, spot_y, spot, c), copy(s, 0, c, 1, s, 2, dev_y, spot_y)

    def relay_x(s, c):
        cond = need(s, spot_y, spot_x, c) & jnp.logical_not(ends_in_x(s, spot_y, c))
        return cond, copy(s, 1, c, 3, s, 3, dev_y, spot_y)

    def relay_y(s, c):
        return need(s, spot_x, spot_y, c) & ends_in_x(s, spot_x, c), copy(s, 2, c, 4, s, 3, dev_x, spot_x)

    def sends(s, c):
        out = [x_copy(s, c), y_copy(s, c), relay_x(s, c), relay_y(s, c)]
        if s < last_of(c):
            out.append(up_copy(s, c))
        return out

    def q_down(i):
        cols = pl.ds(i * WIDE, WIDE)
        return pltpu.make_async_remote_copy(
            src_ref=q_buf.at[:, cols],
            dst_ref=q_up.at[i],
            send_sem=down_send.at[i],
            recv_sem=down_recv.at[i],
            device_id={"seq": dev_down},
            device_id_type=pl.DeviceIdType.MESH,
        )

    ids_down = pltpu.make_async_remote_copy(
        src_ref=ids_buf.at[0, 0],
        dst_ref=ids_up,
        send_sem=down_send.at[SERVED],
        recv_sem=down_recv.at[SERVED],
        device_id={"seq": dev_down},
        device_id_type=pl.DeviceIdType.MESH,
    )

    def part_up(i):
        return [
            pltpu.make_async_remote_copy(
                src_ref=source.at[i],
                dst_ref=target.at[i],
                send_sem=part_send.at[k, i],
                recv_sem=part_recv.at[k, i],
                device_id={"seq": dev_up},
                device_id_type=pl.DeviceIdType.MESH,
            )
            for k, (source, target) in enumerate(((lse_out, lse_in), (part_out, part_in)))
        ]

    def start(pair):
        pl.when(pair[0])(pair[1].start)

    kv_in = [
        pltpu.make_async_copy(kv_hbm.at[:, :, pl.ds(h * DH, DH)], buf.at[0, h, :, 0], in_sem.at[h]) for h in range(HK)
    ]
    ids_in = pltpu.make_async_copy(ids_hbm, ids_buf.at[0, 0], in_sem.at[HK])
    q_in = pltpu.make_async_copy(q_hbm, q_buf, in_sem.at[HK + 1])
    ids_in.start()
    for one in kv_in:
        one.start()
    q_in.start()

    barrier = pltpu.get_barrier_semaphore()
    for cond, device in ((None, dev_x), (None, dev_y), (up_ok, dev_up), (down_ok, dev_down)):
        def greet(device=device):
            pl.semaphore_signal(barrier, inc=1, device_id={"seq": device}, device_id_type=pl.DeviceIdType.MESH)
        if cond is None:
            greet()
        else:
            pl.when(cond)(greet)
    pl.semaphore_wait(barrier, 2 + up_ok.astype(jnp.int32) + down_ok.astype(jnp.int32))

    def gap_of(level, r):
        return SPAN * (level + later(spots[r], spot)) + spot - spots[r]

    def arrive(s, c):
        if s == 0:
            (ids_in if c == IDS else kv_in[c]).wait()
        else:
            pl.when(plane >= s)(functools.partial(wait_slot, s, 0, c))
        if s < last_of(c):
            start(up_copy(s, c))

    def side(s, c):
        start(x_copy(s, c))
        start(y_copy(s, c))

    def relay(s, c):
        for r, one in ((1, relay_x), (2, relay_y)):
            @pl.when(need(s, spot, spots[r], c))
            def _():
                wait_slot(s - later(spots[r], spot), r, c)
            start(one(s, c))

    def wait_diagonal(level, c):
        pl.when(me >= gap_of(level, 3))(functools.partial(wait_slot, level, 3, c))

    def ask():
        q_in.wait()

        @pl.when(down_ok)
        def _():
            ids_down.start()
            for i in range(SERVED):
                q_down(i).start()

    def clear():
        for level in range(top_level + 1):
            for r in range(SPAN if level < top_level else 1):
                @pl.when(me < gap_of(level, r))
                def _():
                    ids_buf[level, r] = jnp.zeros((1, rows), jnp.int32)

                    def body(h, carry):
                        for k in range(2):
                            buf[level, h, k, r] = jnp.zeros((rows, DH), buf.dtype)
                        return carry

                    lax.fori_loop(0, HK, body, 0)

        @pl.when(jnp.logical_not(down_ok))
        def _():
            for i in range(SERVED):
                lse_in[i] = jnp.full((GROUP, rows), NEG_BIG, jnp.float32)
                part_in[i] = jnp.zeros((rows, WIDE), part_in.dtype)

    row = lax.broadcasted_iota(jnp.int32, (rows, rows), 0)
    col = lax.broadcasted_iota(jnp.int32, (rows, rows), 1)

    def blocks_of(level, top):
        out = [(level, r) for r in range(SPAN)]
        return out + [(level + 1, 0)] if level == top - 1 else out

    def fill(table, query_ids, shift, top):
        own = jnp.broadcast_to(query_ids.astype(jnp.float32), (rows, rows)).T
        for level in range(top):
            for place, (lv, r) in enumerate(blocks_of(level, top)):
                gap = gap_of(lv, r)
                limit = jnp.where(me >= gap, WINDOW, 0)
                distance = (gap + shift) * rows + row - col
                other = jnp.broadcast_to(ids_buf[lv, r].astype(jnp.float32), (rows, rows))
                allowed = (own == other) & (distance >= 0) & (distance < limit)
                table[level, :, place * rows:(place + 1) * rows] = jnp.where(allowed, 0.0, NEG_BIG)

    def make_bias():
        for level in range(top_level):
            wait_diagonal(level, IDS)
        fill(bias, ids_buf[0, 0], 0, top_level)

    def make_bias_up():
        @pl.when(up_ok)
        def _():
            ids_down.wait_recv()
            fill(bias_up, ids_up[...], SPAN, top_level - 1)

    def stack(wide):
        return jnp.concatenate([wide[:, g * DH:(g + 1) * DH] for g in range(GROUP)], axis=0)

    def unstack(tall):
        return jnp.concatenate([tall[g * rows:(g + 1) * rows] for g in range(GROUP)], axis=1)

    def attend(q, c, level, top, table, state):
        blocks = blocks_of(level, top)
        span = len(blocks) * rows

        def side_of(k):
            main = buf[level, c, k].reshape(SPAN * rows, DH)
            if len(blocks) == SPAN:
                return main
            return jnp.concatenate([main, buf[level + 1, c, k, 0]], axis=0)

        t = lax.dot_general(q, side_of(0), (((1,), (1,)), ((), ())), preferred_element_type=jnp.float32)
        t = (t * SCALE2).reshape(GROUP, rows, span) + table[level, :, :span][None]
        t = t.reshape(group_rows, span)
        new = jnp.max(t, axis=1, keepdims=True)
        if state is None:
            new = jnp.broadcast_to(new, (group_rows, DH))
        else:
            new = jnp.maximum(state[0], new)
        p = [jnp.exp2(t[:, r * rows:(r + 1) * rows] - new) for r in range(len(blocks))]
        total = functools.reduce(lambda x, y: x + y, p)
        w = jnp.concatenate([one.astype(jnp.bfloat16) for one in p], axis=1)
        acc = jnp.dot(w, side_of(1), preferred_element_type=jnp.float32)
        if state is not None:
            fix = jnp.exp2(state[0] - new)
            total = total + state[1] * fix
            acc = acc + state[2] * fix
        return new, total, acc

    def keep(c, state):
        run_max[c], run_sum[c], run_acc[c] = state

    def kept(c):
        return run_max[c], run_sum[c], run_acc[c]

    def query(c):
        return stack(q_buf[:, c * WIDE:(c + 1) * WIDE])

    def out_copy(c):
        cols = pl.ds(c * WIDE, WIDE)
        return pltpu.make_async_copy(out_buf.at[:, cols], out_hbm.at[:, cols], out_sem.at[c])

    def finish(c, o):
        out_buf[:, c * WIDE:(c + 1) * WIDE] = unstack(o.astype(out_buf.dtype))
        out_copy(c).start()

    def near(c):
        if c >= SERVED:
            wait_diagonal(0, c)
        keep(c, attend(query(c), c, 0, top_level, bias, None))

    def far(c):
        for level in range(1, top_level):
            wait_diagonal(level, c)
            state = attend(query(c), c, level, top_level, bias, kept(c))
            if level < top_level - 1:
                keep(c, state)
        _, total, acc = state
        finish(c, acc / jnp.sum(total, axis=1, keepdims=True))

    def serve(c):
        for level in range(top_level - 1):
            wait_diagonal(level, c)

        @pl.when(up_ok)
        def _():
            q_down(c).wait_recv()
            state = None
            for level in range(top_level - 1):
                state = attend(stack(q_up[c]), c, level, top_level - 1, bias_up, state)
            most, total, acc = state
            total = jnp.sum(total, axis=1, keepdims=True)
            part_out[c] = unstack((acc / total).astype(part_out.dtype))
            lse = most + jnp.log2(total)
            lse_out[c] = jnp.concatenate(
                [
                    jnp.sum(jnp.where(row == col, lse[g * rows:(g + 1) * rows], 0.0), axis=0, keepdims=True)
                    for g in range(GROUP)
                ],
                axis=0,
            )

    def reply(c):
        @pl.when(up_ok)
        def _():
            for one in part_up(c):
                one.start()

    def merge(c):
        @pl.when(down_ok)
        def _():
            for one in part_up(c):
                one.wait_recv()
        most, total, acc = kept(c)
        total = jnp.sum(total, axis=1, keepdims=True)
        other = jnp.concatenate(
            [
                jnp.sum(jnp.where(row == col, lse_in[c, g:g + 1, :], 0.0), axis=1, keepdims=True)
                for g in range(GROUP)
            ],
            axis=0,
        )
        new = jnp.maximum(most, other)
        fix, weight = jnp.exp2(most - new), jnp.exp2(other - new)
        o = acc * fix + stack(part_in[c]).astype(jnp.float32) * weight
        finish(c, o / (total * fix + weight))

    steps = []

    def add(key, what, *args):
        steps.append((key, len(steps), functools.partial(what, *args)))

    served = [c for c in PIECES if c < SERVED]
    whole = [c for c in PIECES if c >= SERVED and c != IDS]
    order = [IDS] + served + whole
    def came(s, c):
        if s == 0:
            return -5.0
        return 1.5 * s if c == IDS else 4.5 * s + order.index(c) - 3.0

    def relayed(s, c):
        if c == IDS:
            return 1.5 * s + 1.0
        return (4.5 if c < SERVED else 5.5) * s + order.index(c)

    for c in order:
        for s in range(last_of(c) + 1):
            add(came(s, c), arrive, s, c)
            add(came(s, c), side, s, c)
            add(relayed(s, c), relay, s, c)
    add(-4, ask)
    add(-3, clear)
    add(relayed(top_level, IDS) + 0.1, make_bias)
    add(relayed(top_level, IDS) + 0.1, make_bias_up)
    for c in served:
        key = max(relayed(top_level - 1, c) + 2, relayed(top_level, IDS) + 0.2)
        add(key, serve, c)
        add(key + 0.1, near, c)
        add(key + 0.2, reply, c)
        add(key + 9, merge, c)
    for c in whole:
        add(max(relayed(1, c) + 1.5, relayed(top_level, IDS) + 0.2), near, c)
        add(relayed(top_level, c) + 2, far, c)
    for _, _, step in sorted(steps, key=lambda one: one[:2]):
        step()

    for c in order:
        for s in range(last_of(c) + 1):
            for cond, one in sends(s, c):
                pl.when(cond)(one.wait_send)

    @pl.when(down_ok)
    def _():
        ids_down.wait_send()
        for i in range(SERVED):
            q_down(i).wait_send()

    @pl.when(up_ok)
    def _():
        for i in range(SERVED):
            for one in part_up(i):
                one.wait_send()

    for c in range(HK):
        out_copy(c).wait()


def solution(mesh):
    n = mesh.shape["seq"]

    def local(queries, keys_values, segment_ids):
        rows = queries.shape[0]
        reach = min(WINDOW, n * rows // 2)
        back = -(-(reach - 1) // rows)
        assert n % SPAN == 0 and back % SPAN == 0 and back >= 2 * SPAN
        levels = back // SPAN
        group_rows = GROUP * rows
        return pl.pallas_call(
            functools.partial(kernel, n, rows, back),
            out_shape=jax.ShapeDtypeStruct(queries.shape, queries.dtype),
            in_specs=[pl.BlockSpec(memory_space=pl.ANY)] * 3,
            out_specs=pl.BlockSpec(memory_space=pl.ANY),
            scratch_shapes=[
                pltpu.VMEM((levels + 1, HK, 2, SPAN, rows, DH), jnp.bfloat16),
                pltpu.VMEM((levels + 1, SPAN, 1, rows), jnp.int32),
                pltpu.VMEM((rows, HQ * DH), jnp.bfloat16),
                pltpu.VMEM((SERVED, rows, WIDE), jnp.bfloat16),
                pltpu.VMEM((1, rows), jnp.int32),
                pltpu.VMEM((rows, HQ * DH), jnp.bfloat16),
                pltpu.VMEM((SERVED, rows, WIDE), jnp.bfloat16),
                pltpu.VMEM((SERVED, rows, WIDE), jnp.bfloat16),
                pltpu.VMEM((SERVED, GROUP, rows), jnp.float32),
                pltpu.VMEM((SERVED, GROUP, rows), jnp.float32),
                pltpu.VMEM((levels, rows, (SPAN + 1) * rows), jnp.float32),
                pltpu.VMEM((levels - 1, rows, (SPAN + 1) * rows), jnp.float32),
                pltpu.VMEM((HK, group_rows, DH), jnp.float32),
                pltpu.VMEM((HK, group_rows, DH), jnp.float32),
                pltpu.VMEM((HK, group_rows, DH), jnp.float32),
                pltpu.SemaphoreType.DMA((HK + 2,)),
                pltpu.SemaphoreType.DMA((HK,)),
                pltpu.SemaphoreType.DMA((levels + 1, 5, HK + 1)),
                pltpu.SemaphoreType.DMA((levels + 1, SPAN, HK + 1)),
                pltpu.SemaphoreType.DMA((SERVED + 1,)),
                pltpu.SemaphoreType.DMA((SERVED + 1,)),
                pltpu.SemaphoreType.DMA((2, SERVED)),
                pltpu.SemaphoreType.DMA((2, SERVED)),
            ],
            compiler_params=pltpu.CompilerParams(
                collective_id=0, has_side_effects=True, vmem_limit_bytes=60 * 1024 * 1024
            ),
        )(queries, keys_values, segment_ids.reshape(1, rows))

    return jax.shard_map(
        local,
        mesh=mesh,
        in_specs=(P(("rep", "seq"), None), P(None, ("rep", "seq"), None), P(("rep", "seq"))),
        out_specs=P(("rep", "seq"), None),
        check_vma=False,
    )
```

```python
import functools
import math

import jax
import jax.numpy as jnp
from jax import lax
from jax.experimental import pallas as pl
from jax.experimental.pallas import tpu as pltpu
from jax.sharding import PartitionSpec as P

HQ = 32
HK = 8
DH = 128
WINDOW = 2048
GROUP = HQ // HK
WIDE = GROUP * DH
SPAN = 4
SERVED = 4
NEG_BIG = -1e30
SCALE2 = DH ** (-0.5) * math.log2(math.e)
IDS = HK
PIECES = [IDS] + list(range(HK))


ORDER = (
    8, 1, 201, 208, 0, 18, 3, 2, 103, 4, 118, 202, 5, 11, 100, 111, 101, 218, 7, 200, 211, 204, 401, 104, 600, 10,
    102, 411, 418, 203, 28, 108, 110, 13, 228, 210, 205, 207, 213, 311, 113, 128, 400, 500, 303, 14, 6, 408, 114, 12,
    428, 206, 112, 301, 15, 214, 212, 402, 308, 410, 106, 105, 404, 318, 403, 17, 117, 300, 314, 217, 215, 24, 25,
    225, 412, 302, 328, 700, 16, 800, 125, 27, 310, 124, 224, 1000, 312, 313, 1001, 107, 1100, 413, 216, 115, 306,
    414, 1002, 901, 26, 417, 424, 325, 116, 226, 1102, 305, 425, 900, 405, 127, 1003, 307, 227, 1103, 304, 902, 324,
    1101, 415, 315, 904, 407, 1200, 426, 406, 903, 316, 416, 1304, 317, 327, 1202, 126, 427, 905, 1305, 1203, 907,
    906, 1307, 326, 1201, 1306,
)


def plain_order(top_level):
    keys = {}
    for c in PIECES:
        top = top_level - 1 if c < SERVED else top_level
        for s in range(top + 1):
            place = s * len(PIECES) + PIECES.index(c)
            for kind in range(3):
                keys[kind * 100 + s * 10 + c] = place
            keys[300 + s * 10 + c] = keys[400 + s * 10 + c] = place + 4
    end = (top_level + 1) * len(PIECES) + 4
    for kind in range(5, 9):
        keys[kind * 100] = end
    for c in range(HK):
        for kind in ((10, 9, 11, 12) if c < SERVED else (9, 13)):
            keys[kind * 100 + c] = end + 1
    for c in range(SERVED):
        keys[1200 + c] = end + 2
        keys[900 + c] = end + 1.5
    return sorted(keys, key=lambda code: (keys[code], code))


def kernel(n, rows, back, q_hbm, kv_hbm, ids_hbm, out_ref, buf, ids_buf, q_buf, q_up, ids_up, part_out, part_in,
           lse_out, lse_in, bias, bias_up, run_max, run_sum, run_acc, in_sem, send_sem, recv_sem, down_send,
           down_recv, part_send, part_recv):
    top_level = back // SPAN
    planes = n // SPAN
    group_rows = GROUP * rows
    me = lax.axis_index("seq")
    plane = me // SPAN
    spot = me % SPAN
    low, high = spot % 2, spot // 2
    spot_x = (1 - low) + 2 * high
    spot_y = low + 2 * (1 - high)
    spot_d = (1 - low) + 2 * (1 - high)
    spots = (spot, spot_x, spot_y, spot_d)
    dev_x = plane * SPAN + spot_x
    dev_y = plane * SPAN + spot_y
    up_ok = plane < planes - 1
    down_ok = plane > 0
    dev_up = jnp.where(up_ok, me + SPAN, me - SPAN)
    dev_down = jnp.where(down_ok, me - SPAN, me + SPAN)

    def last_of(c):
        return top_level - 1 if c < SERVED else top_level

    def later(block, t):
        return (block > t).astype(jnp.int32)

    def need(s, t, block, c):
        gap = SPAN * s + t - block
        return (plane >= s) & (gap >= 1) & (gap <= SPAN * last_of(c))

    def ends_in_x(s, t, c):
        mixed = (t % 2) != (t // 2)
        edge = s == 0 or s == last_of(c)
        if edge:
            return mixed | (c % 2 == 0)
        return jnp.logical_not(mixed) & (c % 2 == 0)

    def ref_of(level, r, c):
        if c == IDS:
            return ids_buf.at[level, r]
        return buf.at[level, c, :, r]

    def copy(s, r, c, lane, to_s, to_r, device, to_spot):
        level, to_level = s - later(spots[r], spot), to_s - later(spots[r], to_spot)
        return pltpu.make_async_remote_copy(
            src_ref=ref_of(level, r, c),
            dst_ref=ref_of(to_level, to_r, c),
            send_sem=send_sem.at[s, lane, c],
            recv_sem=recv_sem.at[to_level, to_r, c],
            device_id={"seq": device},
            device_id_type=pl.DeviceIdType.MESH,
        )

    def wait_slot(level, r, c):
        pltpu.make_async_remote_copy(
            src_ref=ref_of(level, r, c),
            dst_ref=ref_of(level, r, c),
            send_sem=send_sem.at[0, 0, c],
            recv_sem=recv_sem.at[level, r, c],
            device_id={"seq": dev_x},
            device_id_type=pl.DeviceIdType.MESH,
        ).wait_recv()

    def up_copy(s, c):
        return up_ok & (plane >= s), copy(s, 0, c, 2, s + 1, 0, dev_up, spot)

    def x_copy(s, c):
        return need(s, spot_x, spot, c), copy(s, 0, c, 0, s, 1, dev_x, spot_x)

    def y_copy(s, c):
        return need(s, spot_y, spot, c), copy(s, 0, c, 1, s, 2, dev_y, spot_y)

    def relay_x(s, c):
        cond = need(s, spot_y, spot_x, c) & jnp.logical_not(ends_in_x(s, spot_y, c))
        return cond, copy(s, 1, c, 3, s, 3, dev_y, spot_y)

    def relay_y(s, c):
        return need(s, spot_x, spot_y, c) & ends_in_x(s, spot_x, c), copy(s, 2, c, 4, s, 3, dev_x, spot_x)

    def sends(s, c):
        out = [x_copy(s, c), y_copy(s, c), relay_x(s, c), relay_y(s, c)]
        if s < last_of(c):
            out.append(up_copy(s, c))
        return out

    def q_down(i):
        cols = pl.ds(i * WIDE, WIDE)
        return pltpu.make_async_remote_copy(
            src_ref=q_buf.at[:, cols],
            dst_ref=q_up.at[i],
            send_sem=down_send.at[i],
            recv_sem=down_recv.at[i],
            device_id={"seq": dev_down},
            device_id_type=pl.DeviceIdType.MESH,
        )

    ids_down = pltpu.make_async_remote_copy(
        src_ref=ids_buf.at[0, 0],
        dst_ref=ids_up,
        send_sem=down_send.at[SERVED],
        recv_sem=down_recv.at[SERVED],
        device_id={"seq": dev_down},
        device_id_type=pl.DeviceIdType.MESH,
    )

    def part_up(i):
        return [
            pltpu.make_async_remote_copy(
                src_ref=source.at[i],
                dst_ref=target.at[i],
                send_sem=part_send.at[k, i],
                recv_sem=part_recv.at[k, i],
                device_id={"seq": dev_up},
                device_id_type=pl.DeviceIdType.MESH,
            )
            for k, (source, target) in enumerate(((lse_out, lse_in), (part_out, part_in)))
        ]

    def start(pair):
        pl.when(pair[0])(pair[1].start)

    kv_in = [
        pltpu.make_async_copy(kv_hbm.at[:, :, pl.ds(h * DH, DH)], buf.at[0, h, :, 0], in_sem.at[h]) for h in range(HK)
    ]
    ids_in = pltpu.make_async_copy(ids_hbm, ids_buf.at[0, 0], in_sem.at[HK])
    q_in = pltpu.make_async_copy(q_hbm, q_buf, in_sem.at[HK + 1])
    ids_in.start()
    for one in kv_in:
        one.start()
    q_in.start()

    barrier = pltpu.get_barrier_semaphore()
    for cond, device in ((None, dev_x), (None, dev_y), (up_ok, dev_up), (down_ok, dev_down)):
        def greet(device=device):
            pl.semaphore_signal(barrier, inc=1, device_id={"seq": device}, device_id_type=pl.DeviceIdType.MESH)
        if cond is None:
            greet()
        else:
            pl.when(cond)(greet)
    pl.semaphore_wait(barrier, 2 + up_ok.astype(jnp.int32) + down_ok.astype(jnp.int32))

    def gap_of(level, r):
        return SPAN * (level + later(spots[r], spot)) + spot - spots[r]

    def arrive(s, c):
        if s == 0:
            (ids_in if c == IDS else kv_in[c]).wait()
        else:
            pl.when(plane >= s)(functools.partial(wait_slot, s, 0, c))
        if s < last_of(c):
            start(up_copy(s, c))

    def wait_diagonal(level, c):
        pl.when(me >= gap_of(level, 3))(functools.partial(wait_slot, level, 3, c))

    def ask():
        q_in.wait()

        @pl.when(down_ok)
        def _():
            ids_down.start()
            for i in range(SERVED):
                q_down(i).start()

    def clear():
        for level in range(top_level + 1):
            for r in range(SPAN if level < top_level else 1):
                @pl.when(me < gap_of(level, r))
                def _():
                    ids_buf[level, r] = jnp.zeros((1, rows), jnp.int32)

                    def body(h, carry):
                        for k in range(2):
                            buf[level, h, k, r] = jnp.zeros((rows, DH), buf.dtype)
                        return carry

                    lax.fori_loop(0, HK, body, 0)

        @pl.when(jnp.logical_not(down_ok))
        def _():
            for i in range(SERVED):
                lse_in[i] = jnp.full((GROUP, rows), NEG_BIG, jnp.float32)
                part_in[i] = jnp.zeros((rows, WIDE), part_in.dtype)

    row = lax.broadcasted_iota(jnp.int32, (rows, rows), 0)
    col = lax.broadcasted_iota(jnp.int32, (rows, rows), 1)

    def blocks_of(level, top):
        out = [(level, r) for r in range(SPAN)]
        return out + [(level + 1, 0)] if level == top - 1 else out

    def fill(table, query_ids, shift, top):
        own = jnp.broadcast_to(query_ids.astype(jnp.float32), (rows, rows)).T
        for level in range(top):
            for place, (lv, r) in enumerate(blocks_of(level, top)):
                gap = gap_of(lv, r)
                limit = jnp.where(me >= gap, WINDOW, 0)
                distance = (gap + shift) * rows + row - col
                other = jnp.broadcast_to(ids_buf[lv, r].astype(jnp.float32), (rows, rows))
                allowed = (own == other) & (distance >= 0) & (distance < limit)
                table[level, :, place * rows:(place + 1) * rows] = jnp.where(allowed, 0.0, NEG_BIG)

    def make_bias():
        for level in range(top_level):
            wait_diagonal(level, IDS)
        fill(bias, ids_buf[0, 0], 0, top_level)

    def make_bias_up():
        @pl.when(up_ok)
        def _():
            ids_down.wait_recv()
            fill(bias_up, ids_up[...], SPAN, top_level - 1)

    def stack(wide):
        return jnp.concatenate([wide[:, g * DH:(g + 1) * DH] for g in range(GROUP)], axis=0)

    def unstack(tall):
        return jnp.concatenate([tall[g * rows:(g + 1) * rows] for g in range(GROUP)], axis=1)

    def attend(q, c, level, top, table, state):
        blocks = blocks_of(level, top)
        span = len(blocks) * rows

        def side_of(k):
            main = buf[level, c, k].reshape(SPAN * rows, DH)
            if len(blocks) == SPAN:
                return main
            return jnp.concatenate([main, buf[level + 1, c, k, 0]], axis=0)

        t = lax.dot_general(q, side_of(0), (((1,), (1,)), ((), ())), preferred_element_type=jnp.float32)
        t = (t * SCALE2).reshape(GROUP, rows, span) + table[level, :, :span][None]
        t = t.reshape(group_rows, span)
        new = jnp.max(t, axis=1, keepdims=True)
        if state is None:
            new = jnp.broadcast_to(new, (group_rows, DH))
        else:
            new = jnp.maximum(state[0], new)
        p = [jnp.exp2(t[:, r * rows:(r + 1) * rows] - new) for r in range(len(blocks))]
        w = jnp.concatenate([one.astype(jnp.bfloat16) for one in p], axis=1)
        paired = jnp.concatenate([side_of(1), jnp.ones((span, DH), jnp.bfloat16)], axis=1)
        both = jnp.dot(w, paired, preferred_element_type=jnp.float32)
        acc, total = both[:, :DH], both[:, DH:]
        if state is not None:
            fix = jnp.exp2(state[0] - new)
            total = total + state[1] * fix
            acc = acc + state[2] * fix
        return new, total, acc

    def keep(c, state):
        run_max[c], run_sum[c], run_acc[c] = state

    def kept(c):
        return run_max[c], run_sum[c], run_acc[c]

    def query(c):
        return stack(q_buf[:, c * WIDE:(c + 1) * WIDE])

    def finish(c, o):
        out_ref[:, c * WIDE:(c + 1) * WIDE] = unstack(o.astype(out_ref.dtype))

    def near(c):
        if c >= SERVED:
            wait_diagonal(0, c)
        keep(c, attend(query(c), c, 0, top_level, bias, None))

    def far(c):
        for level in range(1, top_level):
            wait_diagonal(level, c)
            state = attend(query(c), c, level, top_level, bias, kept(c))
            if level < top_level - 1:
                keep(c, state)
        _, total, acc = state
        finish(c, acc / total)

    def serve(c):
        for level in range(top_level - 1):
            wait_diagonal(level, c)

        @pl.when(up_ok)
        def _():
            q_down(c).wait_recv()
            state = None
            for level in range(top_level - 1):
                state = attend(stack(q_up[c]), c, level, top_level - 1, bias_up, state)
            most, total, acc = state
            part_out[c] = unstack((acc / total).astype(part_out.dtype))
            lse = most + jnp.log2(total)
            lse_out[c] = jnp.concatenate(
                [
                    jnp.sum(jnp.where(row == col, lse[g * rows:(g + 1) * rows], 0.0), axis=0, keepdims=True)
                    for g in range(GROUP)
                ],
                axis=0,
            )

    def reply(c):
        @pl.when(up_ok)
        def _():
            for one in part_up(c):
                one.start()

    def merge(c):
        @pl.when(down_ok)
        def _():
            for one in part_up(c):
                one.wait_recv()
        most, total, acc = kept(c)
        other = jnp.concatenate(
            [
                jnp.sum(jnp.where(row == col, lse_in[c, g:g + 1, :], 0.0), axis=1, keepdims=True)
                for g in range(GROUP)
            ],
            axis=0,
        )
        new = jnp.maximum(most, other)
        fix, weight = jnp.exp2(most - new), jnp.exp2(other - new)
        o = acc * fix + stack(part_in[c]).astype(jnp.float32) * weight
        finish(c, o / (total * fix + weight))

    def side_x(s, c):
        start(x_copy(s, c))

    def side_y(s, c):
        start(y_copy(s, c))

    def relay(r, one, s, c):
        @pl.when(need(s, spot, spots[r], c))
        def _():
            wait_slot(s - later(spots[r], spot), r, c)
        start(one(s, c))

    actions = (
        arrive, side_x, side_y, functools.partial(relay, 1, relay_x), functools.partial(relay, 2, relay_y),
        lambda s, c: ask(), lambda s, c: clear(), lambda s, c: make_bias(), lambda s, c: make_bias_up(),
        lambda s, c: near(c), lambda s, c: serve(c), lambda s, c: reply(c), lambda s, c: merge(c), lambda s, c: far(c),
    )
    for code in ORDER if top_level == 2 else plain_order(top_level):
        actions[code // 100](code // 10 % 10, code % 10)

    for c in PIECES:
        for s in range(last_of(c) + 1):
            for cond, one in sends(s, c):
                pl.when(cond)(one.wait_send)

    @pl.when(down_ok)
    def _():
        ids_down.wait_send()
        for i in range(SERVED):
            q_down(i).wait_send()

    @pl.when(up_ok)
    def _():
        for i in range(SERVED):
            for one in part_up(i):
                one.wait_send()


def solution(mesh):
    n = mesh.shape["seq"]

    def local(queries, keys_values, segment_ids):
        rows = queries.shape[0]
        reach = min(WINDOW, n * rows // 2)
        back = -(-(reach - 1) // rows)
        assert n % SPAN == 0 and back % SPAN == 0 and back >= 2 * SPAN
        levels = back // SPAN
        group_rows = GROUP * rows
        return pl.pallas_call(
            functools.partial(kernel, n, rows, back),
            out_shape=pltpu.MemorySpace.VMEM(queries.shape, queries.dtype),
            in_specs=[pl.BlockSpec(memory_space=pl.ANY)] * 3,
            out_specs=pl.BlockSpec(memory_space=pltpu.VMEM),
            scratch_shapes=[
                pltpu.VMEM((levels + 1, HK, 2, SPAN, rows, DH), jnp.bfloat16),
                pltpu.VMEM((levels + 1, SPAN, 1, rows), jnp.int32),
                pltpu.VMEM((rows, HQ * DH), jnp.bfloat16),
                pltpu.VMEM((SERVED, rows, WIDE), jnp.bfloat16),
                pltpu.VMEM((1, rows), jnp.int32),
                pltpu.VMEM((SERVED, rows, WIDE), jnp.bfloat16),
                pltpu.VMEM((SERVED, rows, WIDE), jnp.bfloat16),
                pltpu.VMEM((SERVED, GROUP, rows), jnp.float32),
                pltpu.VMEM((SERVED, GROUP, rows), jnp.float32),
                pltpu.VMEM((levels, rows, (SPAN + 1) * rows), jnp.float32),
                pltpu.VMEM((levels - 1, rows, (SPAN + 1) * rows), jnp.float32),
                pltpu.VMEM((HK, group_rows, DH), jnp.float32),
                pltpu.VMEM((HK, group_rows, DH), jnp.float32),
                pltpu.VMEM((HK, group_rows, DH), jnp.float32),
                pltpu.SemaphoreType.DMA((HK + 2,)),
                pltpu.SemaphoreType.DMA((levels + 1, 5, HK + 1)),
                pltpu.SemaphoreType.DMA((levels + 1, SPAN, HK + 1)),
                pltpu.SemaphoreType.DMA((SERVED + 1,)),
                pltpu.SemaphoreType.DMA((SERVED + 1,)),
                pltpu.SemaphoreType.DMA((2, SERVED)),
                pltpu.SemaphoreType.DMA((2, SERVED)),
            ],
            compiler_params=pltpu.CompilerParams(
                collective_id=0, has_side_effects=True, vmem_limit_bytes=60 * 1024 * 1024
            ),
        )(queries, keys_values, segment_ids.reshape(1, rows))

    return jax.shard_map(
        local,
        mesh=mesh,
        in_specs=(P(("rep", "seq"), None), P(None, ("rep", "seq"), None), P(("rep", "seq"))),
        out_specs=P(("rep", "seq"), None),
        check_vma=False,
    )
```

```python
import functools
import math

import jax
import jax.numpy as jnp
from jax import lax
from jax.experimental import pallas as pl
from jax.experimental.pallas import tpu as pltpu
from jax.sharding import PartitionSpec as P

HQ = 32
HK = 8
DH = 128
WINDOW = 2048
GROUP = HQ // HK
WIDE = GROUP * DH
SPAN = 4
SERVED = 5
DETOURED = (6,)
NEG_BIG = -1e30
SCALE2 = DH ** (-0.5) * math.log2(math.e)
NEAR_IDS, FAR_IDS = HK, HK + 1
RIDERS = {0: NEAR_IDS, SERVED: FAR_IDS}


ORDER = (
    0, 100, 1, 101, 2, 200, 3, 103, 203, 500, 102, 4, 204, 10, 110, 210, 104, 5, 202, 201, 400, 6, 206, 11, 211, 111,
    12, 212, 112, 600, 303, 7, 410, 13, 302, 113, 213, 105, 14, 214, 300, 301, 402, 304, 404, 412, 401, 411, 15, 115,
    215, 114, 311, 403, 310, 700, 800, 107, 406, 16, 216, 1000, 900, 414, 313, 17, 217, 205, 413, 312, 116, 1100,
    1002, 902, 207, 106, 25, 225, 1001, 1101, 26, 226, 315, 901, 416, 1102, 314, 125, 305, 117, 1004, 1104, 27, 307,
    227, 1003, 903, 1103, 127, 405, 425, 1200, 126, 1506, 426, 427, 325, 407, 316, 317, 1201, 904, 306, 906, 327,
    1202, 417, 415, 1400, 905, 1305, 1204, 326, 1306, 907, 1307, 1203,
)


def plain_order(top_level):
    keys = {}
    for c in range(HK):
        top = top_level - 1 if c < SERVED else top_level
        for s in range(top + 1):
            place = s * HK + c
            for kind in range(3):
                keys[kind * 100 + s * 10 + c] = place
            keys[300 + s * 10 + c] = keys[400 + s * 10 + c] = place + 4
    end = (top_level + 1) * HK + 4
    for c in DETOURED:
        keys[1500 + c] = HK + c + 8
        keys[300 + c] = keys[310 + c] = HK + c + 12
    for kind in range(5, 9):
        keys[kind * 100] = end
    keys[1400] = end
    for c in range(HK):
        for kind in ((10, 9, 11, 12) if c < SERVED else (9, 13)):
            keys[kind * 100 + c] = end + 1
    for c in range(SERVED):
        keys[1200 + c] = end + 2
        keys[900 + c] = end + 1.5
    return sorted(keys, key=lambda code: (keys[code], code))


def kernel(n, rows, back, q_hbm, kv_hbm, ids_hbm, out_ref, buf, ids_buf, q_buf, q_up, ids_up, part_out, part_in,
           lse_out, lse_in, bias, bias_up, run_max, run_sum, run_acc, in_sem, send_sem, recv_sem, down_send,
           down_recv, part_send, part_recv):
    top_level = back // SPAN
    planes = n // SPAN
    group_rows = GROUP * rows
    me = lax.axis_index("seq")
    plane = me // SPAN
    spot = me % SPAN
    low, high = spot % 2, spot // 2
    spot_x = (1 - low) + 2 * high
    spot_y = low + 2 * (1 - high)
    spot_d = (1 - low) + 2 * (1 - high)
    spots = (spot, spot_x, spot_y, spot_d)
    dev_x = plane * SPAN + spot_x
    dev_y = plane * SPAN + spot_y
    up_ok = plane < planes - 1
    down_ok = plane > 0
    dev_up = jnp.where(up_ok, me + SPAN, me - SPAN)
    dev_down = jnp.where(down_ok, me - SPAN, me + SPAN)

    def last_of(c):
        return top_level - 1 if c < SERVED or c == NEAR_IDS else top_level

    def carrier(c):
        return {NEAR_IDS: 0, FAR_IDS: SERVED}.get(c, c)

    def even(c):
        return carrier(c) % 2 == 0

    def mixed(t):
        return (t % 2) != (t // 2)

    def by_detour(level, t, c):
        return mixed(t) & (level == 0) if carrier(c) in DETOURED else t < 0

    def load(c):
        return [RIDERS[c], c] if c in RIDERS else [c]

    def later(block, t):
        return (block > t).astype(jnp.int32)

    def need(s, t, block, c):
        gap = SPAN * s + t - block
        return (plane >= s) & (gap >= 1) & (gap <= SPAN * last_of(c))

    def ends_in_x(s, t, c):
        edge = s == 0 or s == last_of(c)
        if edge:
            return mixed(t) | even(c)
        return jnp.logical_not(mixed(t)) & even(c)

    def ref_of(level, r, c):
        if c >= HK:
            return ids_buf.at[c - HK, level, r]
        return buf.at[level, c, :, r]

    def copy(s, r, c, lane, to_s, to_r, device, to_spot):
        level, to_level = s - later(spots[r], spot), to_s - later(spots[r], to_spot)
        return pltpu.make_async_remote_copy(
            src_ref=ref_of(level, r, c),
            dst_ref=ref_of(to_level, to_r, c),
            send_sem=send_sem.at[s, lane, c],
            recv_sem=recv_sem.at[to_level, to_r, c],
            device_id={"seq": device},
            device_id_type=pl.DeviceIdType.MESH,
        )

    def wait_slot(level, r, c):
        pltpu.make_async_remote_copy(
            src_ref=ref_of(level, r, c),
            dst_ref=ref_of(level, r, c),
            send_sem=send_sem.at[0, 0, c],
            recv_sem=recv_sem.at[level, r, c],
            device_id={"seq": dev_x},
            device_id_type=pl.DeviceIdType.MESH,
        ).wait_recv()

    def gap_of(level, r):
        return SPAN * (level + later(spots[r], spot)) + spot - spots[r]

    def up_copy(s, c):
        return up_ok & (plane >= s), copy(s, 0, c, 2, s + 1, 0, dev_up, spot)

    def x_copy(s, c):
        direct = jnp.logical_not(by_detour(s - later(spot, spot_x), spot_x, c))
        return need(s, spot_x, spot, c) & direct, copy(s, 0, c, 0, s, 1, dev_x, spot_x)

    def y_copy(s, c):
        return need(s, spot_y, spot, c), copy(s, 0, c, 1, s, 2, dev_y, spot_y)

    def relay_x(s, c):
        cond = need(s, spot_y, spot_x, c) & jnp.logical_not(ends_in_x(s, spot_y, c))
        return cond, copy(s, 1, c, 3, s, 3, dev_y, spot_y)

    def relay_y(s, c):
        return need(s, spot_x, spot_y, c) & ends_in_x(s, spot_x, c), copy(s, 2, c, 4, s, 3, dev_x, spot_x)

    def detour(c):
        s = later(spot_d, spot)
        cond = (me >= gap_of(0, 3)) & need(s, spot_y, spot_d, c) & by_detour(s - later(spot_d, spot_y), spot_y, c)
        return cond, pltpu.make_async_remote_copy(
            src_ref=ref_of(0, 3, c),
            dst_ref=ref_of(s - later(spot_d, spot_y), 1, c),
            send_sem=send_sem.at[0, 5, c],
            recv_sem=recv_sem.at[s - later(spot_d, spot_y), 1, c],
            device_id={"seq": dev_y},
            device_id_type=pl.DeviceIdType.MESH,
        )

    def sends(s, c):
        out = [detour(c)] if s == 0 and carrier(c) in DETOURED else []
        out += [x_copy(s, c), y_copy(s, c), relay_x(s, c), relay_y(s, c)]
        if s < last_of(c):
            out.append(up_copy(s, c))
        return out

    def q_down(i):
        cols = pl.ds(i * WIDE, WIDE)
        return pltpu.make_async_remote_copy(
            src_ref=q_buf.at[:, cols],
            dst_ref=q_up.at[i],
            send_sem=down_send.at[i],
            recv_sem=down_recv.at[i],
            device_id={"seq": dev_down},
            device_id_type=pl.DeviceIdType.MESH,
        )

    ids_down = pltpu.make_async_remote_copy(
        src_ref=ids_buf.at[0, 0, 0],
        dst_ref=ids_up,
        send_sem=down_send.at[SERVED],
        recv_sem=down_recv.at[SERVED],
        device_id={"seq": dev_down},
        device_id_type=pl.DeviceIdType.MESH,
    )

    def part_up(i):
        return [
            pltpu.make_async_remote_copy(
                src_ref=source.at[i],
                dst_ref=target.at[i],
                send_sem=part_send.at[k, i],
                recv_sem=part_recv.at[k, i],
                device_id={"seq": dev_up},
                device_id_type=pl.DeviceIdType.MESH,
            )
            for k, (source, target) in enumerate(((lse_out, lse_in), (part_out, part_in)))
        ]

    def start(pair):
        pl.when(pair[0])(pair[1].start)

    kv_in = [
        pltpu.make_async_copy(kv_hbm.at[:, :, pl.ds(h * DH, DH)], buf.at[0, h, :, 0], in_sem.at[h]) for h in range(HK)
    ]
    ids_in = [pltpu.make_async_copy(ids_hbm, ids_buf.at[k, 0, 0], in_sem.at[HK + k]) for k in range(2)]
    q_in = pltpu.make_async_copy(q_hbm, q_buf, in_sem.at[HK + 2])
    for one in ids_in:
        one.start()
    for one in kv_in:
        one.start()
    q_in.start()

    barrier = pltpu.get_barrier_semaphore()
    for cond, device in ((None, dev_x), (None, dev_y), (up_ok, dev_up), (down_ok, dev_down)):
        def greet(device=device):
            pl.semaphore_signal(barrier, inc=1, device_id={"seq": device}, device_id_type=pl.DeviceIdType.MESH)
        if cond is None:
            greet()
        else:
            pl.when(cond)(greet)
    pl.semaphore_wait(barrier, 2 + up_ok.astype(jnp.int32) + down_ok.astype(jnp.int32))

    def arrive(s, c):
        for k in load(c):
            if s == 0:
                (ids_in[k - HK] if k >= HK else kv_in[k]).wait()
            else:
                pl.when(plane >= s)(functools.partial(wait_slot, s, 0, k))
            if s < last_of(k):
                start(up_copy(s, k))

    def pass_on(c):
        for k in load(c):
            wait_diagonal(0, k)
            start(detour(k))

    def wait_diagonal(level, c):
        pl.when(me >= gap_of(level, 3))(functools.partial(wait_slot, level, 3, c))

    def ask():
        q_in.wait()

        @pl.when(down_ok)
        def _():
            ids_down.start()
            for i in range(SERVED):
                q_down(i).start()

    def clear():
        for level in range(top_level + 1):
            for r in range(SPAN if level < top_level else 1):
                @pl.when(me < gap_of(level, r))
                def _():
                    for k in range(2):
                        ids_buf[k, level, r] = jnp.zeros((1, rows), jnp.int32)

                    def body(h, carry):
                        for k in range(2):
                            buf[level, h, k, r] = jnp.zeros((rows, DH), buf.dtype)
                        return carry

                    lax.fori_loop(0, HK, body, 0)

        @pl.when(jnp.logical_not(down_ok))
        def _():
            for i in range(SERVED):
                lse_in[i] = jnp.full((GROUP, rows), NEG_BIG, jnp.float32)
                part_in[i] = jnp.zeros((rows, WIDE), part_in.dtype)

    row = lax.broadcasted_iota(jnp.int32, (rows, rows), 0)
    col = lax.broadcasted_iota(jnp.int32, (rows, rows), 1)

    def blocks_of(level, top):
        out = [(level, r) for r in range(SPAN)]
        return out + [(level + 1, 0)] if level == top - 1 else out

    def fill(table, known, query_ids, shift, begin, end, top):
        own = jnp.broadcast_to(query_ids.astype(jnp.float32), (rows, rows)).T
        for level in range(begin, end):
            for place, (lv, r) in enumerate(blocks_of(level, top)):
                gap = gap_of(lv, r)
                limit = jnp.where(me >= gap, WINDOW, 0)
                distance = (gap + shift) * rows + row - col
                other = jnp.broadcast_to(ids_buf[known, lv, r].astype(jnp.float32), (rows, rows))
                allowed = (own == other) & (distance >= 0) & (distance < limit)
                table[level, :, place * rows:(place + 1) * rows] = jnp.where(allowed, 0.0, NEG_BIG)

    def make_bias():
        for level in range(top_level - 1):
            wait_diagonal(level, NEAR_IDS)
        fill(bias, 0, ids_buf[0, 0, 0], 0, 0, 1, top_level)

    def make_bias_far():
        for level in range(SERVED in DETOURED, top_level):
            wait_diagonal(level, FAR_IDS)
        fill(bias, 1, ids_buf[0, 0, 0], 0, 1, top_level, top_level)

    def make_bias_up():
        @pl.when(up_ok)
        def _():
            ids_down.wait_recv()
            fill(bias_up, 0, ids_up[...], SPAN, 0, top_level - 1, top_level - 1)

    def stack(wide):
        return jnp.concatenate([wide[:, g * DH:(g + 1) * DH] for g in range(GROUP)], axis=0)

    def unstack(tall):
        return jnp.concatenate([tall[g * rows:(g + 1) * rows] for g in range(GROUP)], axis=1)

    def attend(q, c, level, top, table, state):
        blocks = blocks_of(level, top)
        span = len(blocks) * rows

        def side_of(k):
            main = buf[level, c, k].reshape(SPAN * rows, DH)
            if len(blocks) == SPAN:
                return main
            return jnp.concatenate([main, buf[level + 1, c, k, 0]], axis=0)

        t = lax.dot_general(q, side_of(0), (((1,), (1,)), ((), ())), preferred_element_type=jnp.float32)
        t = (t * SCALE2).reshape(GROUP, rows, span) + table[level, :, :span][None]
        t = t.reshape(group_rows, span)
        new = jnp.max(t, axis=1, keepdims=True)
        if state is None:
            new = jnp.broadcast_to(new, (group_rows, DH))
        else:
            new = jnp.maximum(state[0], new)
        p = [jnp.exp2(t[:, r * rows:(r + 1) * rows] - new) for r in range(len(blocks))]
        w = jnp.concatenate([one.astype(jnp.bfloat16) for one in p], axis=1)
        paired = jnp.concatenate([side_of(1), jnp.ones((span, DH), jnp.bfloat16)], axis=1)
        both = jnp.dot(w, paired, preferred_element_type=jnp.float32)
        acc, total = both[:, :DH], both[:, DH:]
        if state is not None:
            fix = jnp.exp2(state[0] - new)
            total = total + state[1] * fix
            acc = acc + state[2] * fix
        return new, total, acc

    def keep(c, state):
        run_max[c], run_sum[c], run_acc[c] = state

    def kept(c):
        return run_max[c], run_sum[c], run_acc[c]

    def query(c):
        return stack(q_buf[:, c * WIDE:(c + 1) * WIDE])

    def finish(c, o):
        out_ref[:, c * WIDE:(c + 1) * WIDE] = unstack(o.astype(out_ref.dtype))

    def near(c):
        if c >= SERVED and c not in DETOURED:
            wait_diagonal(0, c)
        keep(c, attend(query(c), c, 0, top_level, bias, None))

    def far(c):
        for level in range(1, top_level):
            wait_diagonal(level, c)
            state = attend(query(c), c, level, top_level, bias, kept(c))
            if level < top_level - 1:
                keep(c, state)
        _, total, acc = state
        finish(c, acc / total)

    def serve(c):
        for level in range(top_level - 1):
            wait_diagonal(level, c)

        @pl.when(up_ok)
        def _():
            q_down(c).wait_recv()
            state = None
            for level in range(top_level - 1):
                state = attend(stack(q_up[c]), c, level, top_level - 1, bias_up, state)
            most, total, acc = state
            part_out[c] = unstack((acc / total).astype(part_out.dtype))
            lse = most + jnp.log2(total)
            lse_out[c] = jnp.concatenate(
                [
                    jnp.sum(jnp.where(row == col, lse[g * rows:(g + 1) * rows], 0.0), axis=0, keepdims=True)
                    for g in range(GROUP)
                ],
                axis=0,
            )

    def reply(c):
        @pl.when(up_ok)
        def _():
            for one in part_up(c):
                one.start()

    def merge(c):
        @pl.when(down_ok)
        def _():
            for one in part_up(c):
                one.wait_recv()
        most, total, acc = kept(c)
        other = jnp.concatenate(
            [
                jnp.sum(jnp.where(row == col, lse_in[c, g:g + 1, :], 0.0), axis=1, keepdims=True)
                for g in range(GROUP)
            ],
            axis=0,
        )
        new = jnp.maximum(most, other)
        fix, weight = jnp.exp2(most - new), jnp.exp2(other - new)
        o = acc * fix + stack(part_in[c]).astype(jnp.float32) * weight
        finish(c, o / (total * fix + weight))

    def side_x(s, c):
        for k in load(c):
            start(x_copy(s, k))

    def side_y(s, c):
        for k in load(c):
            start(y_copy(s, k))

    def relay(r, one, s, c):
        for k in load(c):
            @pl.when(need(s, spot, spots[r], k))
            def _():
                wait_slot(s - later(spots[r], spot), r, k)
            start(one(s, k))

    actions = (
        arrive, side_x, side_y, functools.partial(relay, 1, relay_x), functools.partial(relay, 2, relay_y),
        lambda s, c: ask(), lambda s, c: clear(), lambda s, c: make_bias(), lambda s, c: make_bias_up(),
        lambda s, c: near(c), lambda s, c: serve(c), lambda s, c: reply(c), lambda s, c: merge(c), lambda s, c: far(c),
        lambda s, c: make_bias_far(), lambda s, c: pass_on(c),
    )
    def settle():
        for c in range(HK + 2):
            for s in range(last_of(c) + 1):
                for cond, one in sends(s, c):
                    pl.when(cond)(one.wait_send)

        @pl.when(down_ok)
        def _():
            ids_down.wait_send()
            for i in range(SERVED):
                q_down(i).wait_send()

        @pl.when(up_ok)
        def _():
            for i in range(SERVED):
                for one in part_up(i):
                    one.wait_send()

    order = ORDER if top_level == 2 else plain_order(top_level)
    for place, code in enumerate(order):
        if place == len(order) - 1:
            settle()
        actions[code // 100](code // 10 % 10, code % 10)


def solution(mesh):
    n = mesh.shape["seq"]

    def local(queries, keys_values, segment_ids):
        rows = queries.shape[0]
        reach = min(WINDOW, n * rows // 2)
        back = -(-(reach - 1) // rows)
        assert n % SPAN == 0 and back % SPAN == 0 and back >= 2 * SPAN
        levels = back // SPAN
        group_rows = GROUP * rows
        return pl.pallas_call(
            functools.partial(kernel, n, rows, back),
            out_shape=pltpu.MemorySpace.VMEM(queries.shape, queries.dtype),
            in_specs=[pl.BlockSpec(memory_space=pl.ANY)] * 3,
            out_specs=pl.BlockSpec(memory_space=pltpu.VMEM),
            scratch_shapes=[
                pltpu.VMEM((levels + 1, HK, 2, SPAN, rows, DH), jnp.bfloat16),
                pltpu.VMEM((2, levels + 1, SPAN, 1, rows), jnp.int32),
                pltpu.VMEM((rows, HQ * DH), jnp.bfloat16),
                pltpu.VMEM((SERVED, rows, WIDE), jnp.bfloat16),
                pltpu.VMEM((1, rows), jnp.int32),
                pltpu.VMEM((SERVED, rows, WIDE), jnp.bfloat16),
                pltpu.VMEM((SERVED, rows, WIDE), jnp.bfloat16),
                pltpu.VMEM((SERVED, GROUP, rows), jnp.float32),
                pltpu.VMEM((SERVED, GROUP, rows), jnp.float32),
                pltpu.VMEM((levels, rows, (SPAN + 1) * rows), jnp.float32),
                pltpu.VMEM((levels - 1, rows, (SPAN + 1) * rows), jnp.float32),
                pltpu.VMEM((HK, group_rows, DH), jnp.float32),
                pltpu.VMEM((HK, group_rows, DH), jnp.float32),
                pltpu.VMEM((HK, group_rows, DH), jnp.float32),
                pltpu.SemaphoreType.DMA((HK + 3,)),
                pltpu.SemaphoreType.DMA((levels + 1, 6, HK + 2)),
                pltpu.SemaphoreType.DMA((levels + 1, SPAN, HK + 2)),
                pltpu.SemaphoreType.DMA((SERVED + 1,)),
                pltpu.SemaphoreType.DMA((SERVED + 1,)),
                pltpu.SemaphoreType.DMA((2, SERVED)),
                pltpu.SemaphoreType.DMA((2, SERVED)),
            ],
            compiler_params=pltpu.CompilerParams(
                collective_id=0, has_side_effects=True, vmem_limit_bytes=60 * 1024 * 1024
            ),
        )(queries, keys_values, segment_ids.reshape(1, rows))

    return jax.shard_map(
        local,
        mesh=mesh,
        in_specs=(P(("rep", "seq"), None), P(None, ("rep", "seq"), None), P(("rep", "seq"))),
        out_specs=P(("rep", "seq"), None),
        check_vma=False,
    )
```

```python
import functools
import math

import jax
import jax.numpy as jnp
from jax import lax
from jax.experimental import pallas as pl
from jax.experimental.pallas import tpu as pltpu
from jax.sharding import PartitionSpec as P

HQ = 32
HK = 8
DH = 128
WINDOW = 2048
GROUP = HQ // HK
WIDE = GROUP * DH
SPAN = 4
SERVED = 5
DETOURED = (6,)
ENDS_X = (0, 2, 6, 7)
NEG_BIG = -1e30
SCALE2 = DH ** (-0.5) * math.log2(math.e)
NEAR_IDS, FAR_IDS = HK, HK + 1
RIDERS = {0: NEAR_IDS, SERVED: FAR_IDS}


ORDER = (
    0, 200, 1, 101, 500, 2, 202, 102, 100, 4, 104, 6, 10, 110, 210, 206, 201, 204, 106, 11, 111, 211, 400, 5, 105, 12,
    112, 212, 410, 14, 114, 205, 214, 3, 7, 411, 301, 103, 311, 16, 300, 216, 412, 401, 15, 215, 402, 116, 203, 406,
    107, 600, 310, 700, 13, 113, 304, 414, 404, 312, 213, 800, 1000, 17, 217, 314, 302, 1001, 26, 226, 1100, 416,
    1101, 207, 900, 901, 115, 25, 225, 1002, 902, 415, 27, 125, 403, 305, 117, 405, 313, 316, 126, 1102, 227, 127,
    303, 307, 413, 1506, 315, 1004, 1104, 325, 1200, 425, 904, 426, 417, 306, 906, 1201, 407, 1003, 903, 427, 317,
    1202, 905, 1103, 1400, 1305, 326, 1306, 1204, 327, 907, 1307, 1203,
)


def plain_order(top_level):
    keys = {}
    for c in range(HK):
        top = top_level - 1 if c < SERVED else top_level
        for s in range(top + 1):
            place = s * HK + c
            for kind in range(3):
                keys[kind * 100 + s * 10 + c] = place
            keys[300 + s * 10 + c] = keys[400 + s * 10 + c] = place + 4
    end = (top_level + 1) * HK + 4
    for c in DETOURED:
        keys[1500 + c] = HK + c + 8
        keys[300 + c] = keys[310 + c] = HK + c + 12
    for kind in range(5, 9):
        keys[kind * 100] = end
    keys[1400] = end
    for c in range(HK):
        for kind in ((10, 9, 11, 12) if c < SERVED else (9, 13)):
            keys[kind * 100 + c] = end + 1
    for c in range(SERVED):
        keys[1200 + c] = end + 2
        keys[900 + c] = end + 1.5
    return sorted(keys, key=lambda code: (keys[code], code))


def kernel(n, rows, back, q_hbm, kv_hbm, ids_hbm, out_ref, buf, ids_buf, q_buf, q_up, ids_up, part_out, part_in,
           lse_out, lse_in, bias, bias_up, run_max, run_sum, run_acc, in_sem, send_sem, recv_sem, down_send,
           down_recv, part_send, part_recv):
    top_level = back // SPAN
    planes = n // SPAN
    group_rows = GROUP * rows
    me = lax.axis_index("seq")
    plane = me // SPAN
    spot = me % SPAN
    low, high = spot % 2, spot // 2
    spot_x = (1 - low) + 2 * high
    spot_y = low + 2 * (1 - high)
    spot_d = (1 - low) + 2 * (1 - high)
    spots = (spot, spot_x, spot_y, spot_d)
    dev_x = plane * SPAN + spot_x
    dev_y = plane * SPAN + spot_y
    up_ok = plane < planes - 1
    down_ok = plane > 0
    dev_up = jnp.where(up_ok, me + SPAN, me - SPAN)
    dev_down = jnp.where(down_ok, me - SPAN, me + SPAN)

    def last_of(c):
        return top_level - 1 if c < SERVED or c == NEAR_IDS else top_level

    def carrier(c):
        return {NEAR_IDS: 0, FAR_IDS: SERVED}.get(c, c)

    def chosen(c):
        return carrier(c) in ENDS_X

    def mixed(t):
        return (t % 2) != (t // 2)

    def by_detour(level, t, c):
        return mixed(t) & (level == 0) if carrier(c) in DETOURED else t < 0

    def load(c):
        return [RIDERS[c], c] if c in RIDERS else [c]

    def later(block, t):
        return (block > t).astype(jnp.int32)

    def need(s, t, block, c):
        gap = SPAN * s + t - block
        return (plane >= s) & (gap >= 1) & (gap <= SPAN * last_of(c))

    def ends_in_x(s, t, c):
        edge = s == 0 or s == last_of(c)
        if edge:
            return mixed(t) | chosen(c)
        return jnp.logical_not(mixed(t)) & chosen(c)

    def ref_of(level, r, c):
        if c >= HK:
            return ids_buf.at[c - HK, level, r]
        return buf.at[level, c, r]

    def copy(s, r, c, lane, to_s, to_r, device, to_spot):
        level, to_level = s - later(spots[r], spot), to_s - later(spots[r], to_spot)
        return pltpu.make_async_remote_copy(
            src_ref=ref_of(level, r, c),
            dst_ref=ref_of(to_level, to_r, c),
            send_sem=send_sem.at[s, lane, c],
            recv_sem=recv_sem.at[to_level, to_r, c],
            device_id={"seq": device},
            device_id_type=pl.DeviceIdType.MESH,
        )

    def wait_slot(level, r, c):
        pltpu.make_async_remote_copy(
            src_ref=ref_of(level, r, c),
            dst_ref=ref_of(level, r, c),
            send_sem=send_sem.at[0, 0, c],
            recv_sem=recv_sem.at[level, r, c],
            device_id={"seq": dev_x},
            device_id_type=pl.DeviceIdType.MESH,
        ).wait_recv()

    def gap_of(level, r):
        return SPAN * (level + later(spots[r], spot)) + spot - spots[r]

    def up_copy(s, c):
        return up_ok & (plane >= s), copy(s, 0, c, 2, s + 1, 0, dev_up, spot)

    def x_copy(s, c):
        direct = jnp.logical_not(by_detour(s - later(spot, spot_x), spot_x, c))
        return need(s, spot_x, spot, c) & direct, copy(s, 0, c, 0, s, 1, dev_x, spot_x)

    def y_copy(s, c):
        return need(s, spot_y, spot, c), copy(s, 0, c, 1, s, 2, dev_y, spot_y)

    def relay_x(s, c):
        cond = need(s, spot_y, spot_x, c) & jnp.logical_not(ends_in_x(s, spot_y, c))
        return cond, copy(s, 1, c, 3, s, 3, dev_y, spot_y)

    def relay_y(s, c):
        return need(s, spot_x, spot_y, c) & ends_in_x(s, spot_x, c), copy(s, 2, c, 4, s, 3, dev_x, spot_x)

    def detour(c):
        s = later(spot_d, spot)
        cond = (me >= gap_of(0, 3)) & need(s, spot_y, spot_d, c) & by_detour(s - later(spot_d, spot_y), spot_y, c)
        return cond, pltpu.make_async_remote_copy(
            src_ref=ref_of(0, 3, c),
            dst_ref=ref_of(s - later(spot_d, spot_y), 1, c),
            send_sem=send_sem.at[0, 5, c],
            recv_sem=recv_sem.at[s - later(spot_d, spot_y), 1, c],
            device_id={"seq": dev_y},
            device_id_type=pl.DeviceIdType.MESH,
        )

    def sends(s, c):
        out = [detour(c)] if s == 0 and carrier(c) in DETOURED else []
        out += [x_copy(s, c), y_copy(s, c), relay_x(s, c), relay_y(s, c)]
        if s < last_of(c):
            out.append(up_copy(s, c))
        return out

    def q_down(i):
        cols = pl.ds(i * WIDE, WIDE)
        return pltpu.make_async_remote_copy(
            src_ref=q_buf.at[:, cols],
            dst_ref=q_up.at[i],
            send_sem=down_send.at[i],
            recv_sem=down_recv.at[i],
            device_id={"seq": dev_down},
            device_id_type=pl.DeviceIdType.MESH,
        )

    ids_down = pltpu.make_async_remote_copy(
        src_ref=ids_buf.at[0, 0, 0],
        dst_ref=ids_up,
        send_sem=down_send.at[SERVED],
        recv_sem=down_recv.at[SERVED],
        device_id={"seq": dev_down},
        device_id_type=pl.DeviceIdType.MESH,
    )

    def part_up(i):
        return [
            pltpu.make_async_remote_copy(
                src_ref=source.at[i],
                dst_ref=target.at[i],
                send_sem=part_send.at[k, i],
                recv_sem=part_recv.at[k, i],
                device_id={"seq": dev_up},
                device_id_type=pl.DeviceIdType.MESH,
            )
            for k, (source, target) in enumerate(((lse_out, lse_in), (part_out, part_in)))
        ]

    def start(pair):
        pl.when(pair[0])(pair[1].start)

    kv_in = [
        pltpu.make_async_copy(kv_hbm.at[:, :, pl.ds(h * DH, DH)], buf.at[0, h, 0], in_sem.at[h]) for h in range(HK)
    ]
    ids_in = [pltpu.make_async_copy(ids_hbm, ids_buf.at[k, 0, 0], in_sem.at[HK + k]) for k in range(2)]
    q_in = pltpu.make_async_copy(q_hbm, q_buf, in_sem.at[HK + 2])
    for one in ids_in:
        one.start()
    for one in kv_in:
        one.start()
    q_in.start()

    barrier = pltpu.get_barrier_semaphore()
    for cond, device in ((None, dev_x), (None, dev_y), (up_ok, dev_up), (down_ok, dev_down)):
        def greet(device=device):
            pl.semaphore_signal(barrier, inc=1, device_id={"seq": device}, device_id_type=pl.DeviceIdType.MESH)
        if cond is None:
            greet()
        else:
            pl.when(cond)(greet)
    pl.semaphore_wait(barrier, 2 + up_ok.astype(jnp.int32) + down_ok.astype(jnp.int32))

    def arrive(s, c):
        for k in load(c):
            if s == 0:
                (ids_in[k - HK] if k >= HK else kv_in[k]).wait()
            else:
                pl.when(plane >= s)(functools.partial(wait_slot, s, 0, k))
            if s < last_of(k):
                start(up_copy(s, k))

    def pass_on(c):
        for k in load(c):
            wait_diagonal(0, k)
            start(detour(k))

    def wait_diagonal(level, c):
        pl.when(me >= gap_of(level, 3))(functools.partial(wait_slot, level, 3, c))

    def ask():
        q_in.wait()

        @pl.when(down_ok)
        def _():
            ids_down.start()
            for i in range(SERVED):
                q_down(i).start()

    def clear():
        for level in range(top_level + 1):
            for r in range(SPAN if level < top_level else 1):
                @pl.when(me < gap_of(level, r))
                def _():
                    for k in range(2):
                        ids_buf[k, level, r] = jnp.zeros((1, rows), jnp.int32)

                    def body(h, carry):
                        for k in range(2):
                            buf[level, h, r, k] = jnp.zeros((rows, DH), buf.dtype)
                        return carry

                    lax.fori_loop(0, HK, body, 0)

        @pl.when(jnp.logical_not(down_ok))
        def _():
            for i in range(SERVED):
                lse_in[i] = jnp.full((GROUP, rows), NEG_BIG, jnp.float32)
                part_in[i] = jnp.zeros((rows, WIDE), part_in.dtype)

    row = lax.broadcasted_iota(jnp.int32, (rows, rows), 0)
    col = lax.broadcasted_iota(jnp.int32, (rows, rows), 1)

    def blocks_of(level, top):
        out = [(level, r) for r in range(SPAN)]
        return out + [(level + 1, 0)] if level == top - 1 else out

    def fill(table, known, query_ids, shift, begin, end, top):
        own = jnp.broadcast_to(query_ids.astype(jnp.float32), (rows, rows)).T
        for level in range(begin, end):
            for place, (lv, r) in enumerate(blocks_of(level, top)):
                gap = gap_of(lv, r)
                limit = jnp.where(me >= gap, WINDOW, 0)
                distance = (gap + shift) * rows + row - col
                other = jnp.broadcast_to(ids_buf[known, lv, r].astype(jnp.float32), (rows, rows))
                allowed = (own == other) & (distance >= 0) & (distance < limit)
                table[level, :, place * rows:(place + 1) * rows] = jnp.where(allowed, 0.0, NEG_BIG)

    def make_bias():
        for level in range(top_level - 1):
            wait_diagonal(level, NEAR_IDS)
        fill(bias, 0, ids_buf[0, 0, 0], 0, 0, 1, top_level)

    def make_bias_far():
        for level in range(SERVED in DETOURED, top_level):
            wait_diagonal(level, FAR_IDS)
        fill(bias, 1, ids_buf[0, 0, 0], 0, 1, top_level, top_level)

    def make_bias_up():
        @pl.when(up_ok)
        def _():
            ids_down.wait_recv()
            fill(bias_up, 0, ids_up[...], SPAN, 0, top_level - 1, top_level - 1)

    def stack(wide):
        return jnp.concatenate([wide[:, g * DH:(g + 1) * DH] for g in range(GROUP)], axis=0)

    def unstack(tall):
        return jnp.concatenate([tall[g * rows:(g + 1) * rows] for g in range(GROUP)], axis=1)

    def attend(q, c, level, top, table, state):
        blocks = blocks_of(level, top)
        span = len(blocks) * rows

        def side_of(k):
            main = buf[level, c, :, k].reshape(SPAN * rows, DH)
            if len(blocks) == SPAN:
                return main
            return jnp.concatenate([main, buf[level + 1, c, 0, k]], axis=0)

        t = lax.dot_general(q, side_of(0), (((1,), (1,)), ((), ())), preferred_element_type=jnp.float32)
        t = (t * SCALE2).reshape(GROUP, rows, span) + table[level, :, :span][None]
        t = t.reshape(group_rows, span)
        new = jnp.max(t, axis=1, keepdims=True)
        if state is None:
            new = jnp.broadcast_to(new, (group_rows, DH))
        else:
            new = jnp.maximum(state[0], new)
        p = [jnp.exp2(t[:, r * rows:(r + 1) * rows] - new) for r in range(len(blocks))]
        w = jnp.concatenate([one.astype(jnp.bfloat16) for one in p], axis=1)
        paired = jnp.concatenate([side_of(1), jnp.ones((span, DH), jnp.bfloat16)], axis=1)
        both = jnp.dot(w, paired, preferred_element_type=jnp.float32)
        acc, total = both[:, :DH], both[:, DH:]
        if state is not None:
            fix = jnp.exp2(state[0] - new)
            total = total + state[1] * fix
            acc = acc + state[2] * fix
        return new, total, acc

    def keep(c, state):
        run_max[c], run_sum[c], run_acc[c] = state

    def kept(c):
        return run_max[c], run_sum[c], run_acc[c]

    def query(c):
        return stack(q_buf[:, c * WIDE:(c + 1) * WIDE])

    def finish(c, o):
        out_ref[:, c * WIDE:(c + 1) * WIDE] = unstack(o.astype(out_ref.dtype))

    def near(c):
        if c >= SERVED and c not in DETOURED:
            wait_diagonal(0, c)
        keep(c, attend(query(c), c, 0, top_level, bias, None))

    def far(c):
        for level in range(1, top_level):
            wait_diagonal(level, c)
            state = attend(query(c), c, level, top_level, bias, kept(c))
            if level < top_level - 1:
                keep(c, state)
        _, total, acc = state
        finish(c, acc / total)

    def serve(c):
        for level in range(top_level - 1):
            wait_diagonal(level, c)

        @pl.when(up_ok)
        def _():
            q_down(c).wait_recv()
            state = None
            for level in range(top_level - 1):
                state = attend(stack(q_up[c]), c, level, top_level - 1, bias_up, state)
            most, total, acc = state
            part_out[c] = unstack((acc / total).astype(part_out.dtype))
            lse = most + jnp.log2(total)
            lse_out[c] = jnp.concatenate(
                [
                    jnp.sum(jnp.where(row == col, lse[g * rows:(g + 1) * rows], 0.0), axis=0, keepdims=True)
                    for g in range(GROUP)
                ],
                axis=0,
            )

    def reply(c):
        @pl.when(up_ok)
        def _():
            for one in part_up(c):
                one.start()

    def merge(c):
        @pl.when(down_ok)
        def _():
            for one in part_up(c):
                one.wait_recv()
        most, total, acc = kept(c)
        other = jnp.concatenate(
            [
                jnp.sum(jnp.where(row == col, lse_in[c, g:g + 1, :], 0.0), axis=1, keepdims=True)
                for g in range(GROUP)
            ],
            axis=0,
        )
        new = jnp.maximum(most, other)
        fix, weight = jnp.exp2(most - new), jnp.exp2(other - new)
        o = acc * fix + stack(part_in[c]).astype(jnp.float32) * weight
        finish(c, o / (total * fix + weight))

    def side_x(s, c):
        for k in load(c):
            start(x_copy(s, k))

    def side_y(s, c):
        for k in load(c):
            start(y_copy(s, k))

    def relay(r, one, s, c):
        for k in load(c):
            @pl.when(need(s, spot, spots[r], k))
            def _():
                wait_slot(s - later(spots[r], spot), r, k)
            start(one(s, k))

    actions = (
        arrive, side_x, side_y, functools.partial(relay, 1, relay_x), functools.partial(relay, 2, relay_y),
        lambda s, c: ask(), lambda s, c: clear(), lambda s, c: make_bias(), lambda s, c: make_bias_up(),
        lambda s, c: near(c), lambda s, c: serve(c), lambda s, c: reply(c), lambda s, c: merge(c), lambda s, c: far(c),
        lambda s, c: make_bias_far(), lambda s, c: pass_on(c),
    )
    def settle():
        for c in range(HK + 2):
            for s in range(last_of(c) + 1):
                for cond, one in sends(s, c):
                    pl.when(cond)(one.wait_send)

        @pl.when(down_ok)
        def _():
            ids_down.wait_send()
            for i in range(SERVED):
                q_down(i).wait_send()

        @pl.when(up_ok)
        def _():
            for i in range(SERVED):
                for one in part_up(i):
                    one.wait_send()

    order = ORDER if top_level == 2 else plain_order(top_level)
    for place, code in enumerate(order):
        if place == len(order) - 1:
            settle()
        actions[code // 100](code // 10 % 10, code % 10)


def solution(mesh):
    n = mesh.shape["seq"]

    def local(queries, keys_values, segment_ids):
        rows = queries.shape[0]
        reach = min(WINDOW, n * rows // 2)
        back = -(-(reach - 1) // rows)
        assert n % SPAN == 0 and back % SPAN == 0 and back >= 2 * SPAN
        levels = back // SPAN
        group_rows = GROUP * rows
        return pl.pallas_call(
            functools.partial(kernel, n, rows, back),
            out_shape=pltpu.MemorySpace.VMEM(queries.shape, queries.dtype),
            in_specs=[pl.BlockSpec(memory_space=pl.ANY)] * 3,
            out_specs=pl.BlockSpec(memory_space=pltpu.VMEM),
            scratch_shapes=[
                pltpu.VMEM((levels + 1, HK, SPAN, 2, rows, DH), jnp.bfloat16),
                pltpu.VMEM((2, levels + 1, SPAN, 1, rows), jnp.int32),
                pltpu.VMEM((rows, HQ * DH), jnp.bfloat16),
                pltpu.VMEM((SERVED, rows, WIDE), jnp.bfloat16),
                pltpu.VMEM((1, rows), jnp.int32),
                pltpu.VMEM((SERVED, rows, WIDE), jnp.bfloat16),
                pltpu.VMEM((SERVED, rows, WIDE), jnp.bfloat16),
                pltpu.VMEM((SERVED, GROUP, rows), jnp.float32),
                pltpu.VMEM((SERVED, GROUP, rows), jnp.float32),
                pltpu.VMEM((levels, rows, (SPAN + 1) * rows), jnp.float32),
                pltpu.VMEM((levels - 1, rows, (SPAN + 1) * rows), jnp.float32),
                pltpu.VMEM((HK, group_rows, DH), jnp.float32),
                pltpu.VMEM((HK, group_rows, DH), jnp.float32),
                pltpu.VMEM((HK, group_rows, DH), jnp.float32),
                pltpu.SemaphoreType.DMA((HK + 3,)),
                pltpu.SemaphoreType.DMA((levels + 1, 6, HK + 2)),
                pltpu.SemaphoreType.DMA((levels + 1, SPAN, HK + 2)),
                pltpu.SemaphoreType.DMA((SERVED + 1,)),
                pltpu.SemaphoreType.DMA((SERVED + 1,)),
                pltpu.SemaphoreType.DMA((2, SERVED)),
                pltpu.SemaphoreType.DMA((2, SERVED)),
            ],
            compiler_params=pltpu.CompilerParams(
                collective_id=0, has_side_effects=True, vmem_limit_bytes=60 * 1024 * 1024
            ),
        )(queries, keys_values, segment_ids.reshape(1, rows))

    return jax.shard_map(
        local,
        mesh=mesh,
        in_specs=(P(("rep", "seq"), None), P(None, ("rep", "seq"), None), P(("rep", "seq"))),
        out_specs=P(("rep", "seq"), None),
        check_vma=False,
    )
```

```python
import functools
import math

import jax
import jax.numpy as jnp
from jax import lax
from jax.experimental import pallas as pl
from jax.experimental.pallas import tpu as pltpu
from jax.sharding import PartitionSpec as P

HQ = 32
HK = 8
DH = 128
WINDOW = 2048
GROUP = HQ // HK
WIDE = GROUP * DH
SPAN = 4
SERVED = 5
DETOURED = (6,)
ENDS_X = (0, 2, 6, 7)
NEG_BIG = -1e30
SCALE2 = DH ** (-0.5) * math.log2(math.e)
NEAR_IDS, FAR_IDS = HK, HK + 1
RIDERS = {0: NEAR_IDS, SERVED: FAR_IDS}


ORDER = (
    0, 200, 1, 101, 500, 2, 202, 102, 100, 4, 104, 6, 10, 110, 210, 206, 201, 204, 106, 11, 111, 211, 400, 5, 105, 12,
    112, 212, 410, 14, 114, 205, 214, 3, 7, 411, 301, 103, 311, 16, 300, 216, 412, 401, 15, 215, 402, 116, 203, 406,
    107, 600, 310, 700, 13, 113, 304, 414, 404, 312, 213, 800, 1000, 17, 217, 314, 302, 1001, 26, 226, 1100, 416,
    1101, 207, 900, 901, 115, 25, 225, 1002, 902, 415, 27, 125, 403, 305, 117, 405, 313, 316, 126, 1102, 227, 127,
    303, 307, 413, 1506, 315, 1004, 1104, 325, 1200, 425, 904, 426, 417, 306, 906, 1201, 407, 1003, 903, 427, 317,
    1202, 905, 1103, 1400, 1305, 326, 1306, 1204, 327, 907, 1307, 1203,
)


def plain_order(top_level):
    keys = {}
    for c in range(HK):
        top = top_level - 1 if c < SERVED else top_level
        for s in range(top + 1):
            place = s * HK + c
            for kind in range(3):
                keys[kind * 100 + s * 10 + c] = place
            keys[300 + s * 10 + c] = keys[400 + s * 10 + c] = place + 4
    end = (top_level + 1) * HK + 4
    for c in DETOURED:
        keys[1500 + c] = HK + c + 8
        keys[300 + c] = keys[310 + c] = HK + c + 12
    for kind in range(5, 9):
        keys[kind * 100] = end
    keys[1400] = end
    for c in range(HK):
        for kind in ((10, 9, 11, 12) if c < SERVED else (9, 13)):
            keys[kind * 100 + c] = end + 1
    for c in range(SERVED):
        keys[1200 + c] = end + 2
        keys[900 + c] = end + 1.5
    return sorted(keys, key=lambda code: (keys[code], code))


def kernel(n, rows, back, q_hbm, kv_hbm, ids_hbm, out_ref, buf, ids_buf, q_buf, q_up, ids_up, part_out, part_in,
           lse_out, lse_in, bias, bias_up, run_max, run_sum, run_acc, in_sem, send_sem, recv_sem, down_send,
           down_recv, part_send, part_recv):
    top_level = back // SPAN
    planes = n // SPAN
    group_rows = GROUP * rows
    me = lax.axis_index("seq")
    plane = me // SPAN
    spot = me % SPAN
    low, high = spot % 2, spot // 2
    spot_x = (1 - low) + 2 * high
    spot_y = low + 2 * (1 - high)
    spot_d = (1 - low) + 2 * (1 - high)
    spots = (spot, spot_x, spot_y, spot_d)
    dev_x = plane * SPAN + spot_x
    dev_y = plane * SPAN + spot_y
    up_ok = plane < planes - 1
    down_ok = plane > 0
    dev_up = jnp.where(up_ok, me + SPAN, me - SPAN)
    dev_down = jnp.where(down_ok, me - SPAN, me + SPAN)

    def last_of(c):
        return top_level - 1 if c < SERVED or c == NEAR_IDS else top_level

    def carrier(c):
        return {NEAR_IDS: 0, FAR_IDS: SERVED}.get(c, c)

    def chosen(c):
        return carrier(c) in ENDS_X

    def mixed(t):
        return (t % 2) != (t // 2)

    def by_detour(level, t, c):
        return mixed(t) & (level == 0) if carrier(c) in DETOURED else t < 0

    def load(c):
        return [RIDERS[c], c] if c in RIDERS else [c]

    def later(block, t):
        return (block > t).astype(jnp.int32)

    def need(s, t, block, c):
        gap = SPAN * s + t - block
        return (plane >= s) & (gap >= 1) & (gap <= SPAN * last_of(c))

    def ends_in_x(s, t, c):
        edge = s == 0 or s == last_of(c)
        if edge:
            return mixed(t) | chosen(c)
        return jnp.logical_not(mixed(t)) & chosen(c)

    def ref_of(level, r, c):
        if c >= HK:
            return ids_buf.at[c - HK, level, r]
        return buf.at[level, c, r]

    def copy(s, r, c, lane, to_s, to_r, device, to_spot):
        level, to_level = s - later(spots[r], spot), to_s - later(spots[r], to_spot)
        return pltpu.make_async_remote_copy(
            src_ref=ref_of(level, r, c),
            dst_ref=ref_of(to_level, to_r, c),
            send_sem=send_sem.at[s, lane, c],
            recv_sem=recv_sem.at[to_level, to_r, c],
            device_id={"seq": device},
            device_id_type=pl.DeviceIdType.MESH,
        )

    def wait_slot(level, r, c):
        pltpu.make_async_remote_copy(
            src_ref=ref_of(level, r, c),
            dst_ref=ref_of(level, r, c),
            send_sem=send_sem.at[0, 0, c],
            recv_sem=recv_sem.at[level, r, c],
            device_id={"seq": dev_x},
            device_id_type=pl.DeviceIdType.MESH,
        ).wait_recv()

    def gap_of(level, r):
        return SPAN * (level + later(spots[r], spot)) + spot - spots[r]

    def arrives(s, at, c):
        if c < SERVED and s == last_of(c):
            return (at >= s) & ((at < planes - 1) | (spot > 0))
        return at >= s

    def up_copy(s, c):
        return up_ok & (plane >= s) & arrives(s + 1, plane + 1, c), copy(s, 0, c, 2, s + 1, 0, dev_up, spot)

    def x_copy(s, c):
        direct = jnp.logical_not(by_detour(s - later(spot, spot_x), spot_x, c))
        return need(s, spot_x, spot, c) & direct, copy(s, 0, c, 0, s, 1, dev_x, spot_x)

    def y_copy(s, c):
        return need(s, spot_y, spot, c), copy(s, 0, c, 1, s, 2, dev_y, spot_y)

    def relay_x(s, c):
        cond = need(s, spot_y, spot_x, c) & jnp.logical_not(ends_in_x(s, spot_y, c))
        return cond, copy(s, 1, c, 3, s, 3, dev_y, spot_y)

    def relay_y(s, c):
        return need(s, spot_x, spot_y, c) & ends_in_x(s, spot_x, c), copy(s, 2, c, 4, s, 3, dev_x, spot_x)

    def detour(c):
        s = later(spot_d, spot)
        cond = (me >= gap_of(0, 3)) & need(s, spot_y, spot_d, c) & by_detour(s - later(spot_d, spot_y), spot_y, c)
        return cond, pltpu.make_async_remote_copy(
            src_ref=ref_of(0, 3, c),
            dst_ref=ref_of(s - later(spot_d, spot_y), 1, c),
            send_sem=send_sem.at[0, 5, c],
            recv_sem=recv_sem.at[s - later(spot_d, spot_y), 1, c],
            device_id={"seq": dev_y},
            device_id_type=pl.DeviceIdType.MESH,
        )

    def sends(s, c):
        out = [detour(c)] if s == 0 and carrier(c) in DETOURED else []
        out += [x_copy(s, c), y_copy(s, c), relay_x(s, c), relay_y(s, c)]
        if s < last_of(c):
            out.append(up_copy(s, c))
        return out

    def q_down(i):
        cols = pl.ds(i * WIDE, WIDE)
        return pltpu.make_async_remote_copy(
            src_ref=q_buf.at[:, cols],
            dst_ref=q_up.at[i],
            send_sem=down_send.at[i],
            recv_sem=down_recv.at[i],
            device_id={"seq": dev_down},
            device_id_type=pl.DeviceIdType.MESH,
        )

    ids_down = pltpu.make_async_remote_copy(
        src_ref=ids_buf.at[0, 0, 0],
        dst_ref=ids_up,
        send_sem=down_send.at[SERVED],
        recv_sem=down_recv.at[SERVED],
        device_id={"seq": dev_down},
        device_id_type=pl.DeviceIdType.MESH,
    )

    def part_up(i):
        return [
            pltpu.make_async_remote_copy(
                src_ref=source.at[i],
                dst_ref=target.at[i],
                send_sem=part_send.at[k, i],
                recv_sem=part_recv.at[k, i],
                device_id={"seq": dev_up},
                device_id_type=pl.DeviceIdType.MESH,
            )
            for k, (source, target) in enumerate(((lse_out, lse_in), (part_out, part_in)))
        ]

    def start(pair):
        pl.when(pair[0])(pair[1].start)

    kv_in = [
        pltpu.make_async_copy(kv_hbm.at[:, :, pl.ds(h * DH, DH)], buf.at[0, h, 0], in_sem.at[h]) for h in range(HK)
    ]
    ids_in = [pltpu.make_async_copy(ids_hbm, ids_buf.at[k, 0, 0], in_sem.at[HK + k]) for k in range(2)]
    q_in = pltpu.make_async_copy(q_hbm, q_buf, in_sem.at[HK + 2])
    for one in ids_in:
        one.start()
    for one in kv_in:
        one.start()
    q_in.start()

    barrier = pltpu.get_barrier_semaphore()
    for cond, device in ((None, dev_x), (None, dev_y), (up_ok, dev_up), (down_ok, dev_down)):
        def greet(device=device):
            pl.semaphore_signal(barrier, inc=1, device_id={"seq": device}, device_id_type=pl.DeviceIdType.MESH)
        if cond is None:
            greet()
        else:
            pl.when(cond)(greet)
    pl.semaphore_wait(barrier, 2 + up_ok.astype(jnp.int32) + down_ok.astype(jnp.int32))

    def arrive(s, c):
        for k in load(c):
            if s == 0:
                (ids_in[k - HK] if k >= HK else kv_in[k]).wait()
            else:
                pl.when(arrives(s, plane, k))(functools.partial(wait_slot, s, 0, k))
            if s < last_of(k):
                start(up_copy(s, k))

    def pass_on(c):
        for k in load(c):
            wait_diagonal(0, k)
            start(detour(k))

    def wait_diagonal(level, c):
        pl.when(me >= gap_of(level, 3))(functools.partial(wait_slot, level, 3, c))

    def ask():
        q_in.wait()

        @pl.when(down_ok)
        def _():
            ids_down.start()
            for i in range(SERVED):
                q_down(i).start()

    def clear():
        for level in range(top_level + 1):
            for r in range(SPAN if level < top_level else 1):
                @pl.when(me < gap_of(level, r))
                def _():
                    for k in range(2):
                        ids_buf[k, level, r] = jnp.zeros((1, rows), jnp.int32)

                    def body(h, carry):
                        for k in range(2):
                            buf[level, h, r, k] = jnp.zeros((rows, DH), buf.dtype)
                        return carry

                    lax.fori_loop(0, HK, body, 0)

        @pl.when(jnp.logical_not(down_ok))
        def _():
            for i in range(SERVED):
                lse_in[i] = jnp.full((GROUP, rows), NEG_BIG, jnp.float32)
                part_in[i] = jnp.zeros((rows, WIDE), part_in.dtype)

    row = lax.broadcasted_iota(jnp.int32, (rows, rows), 0)
    col = lax.broadcasted_iota(jnp.int32, (rows, rows), 1)

    def blocks_of(level, top):
        out = [(level, r) for r in range(SPAN)]
        return out + [(level + 1, 0)] if level == top - 1 else out

    def fill(table, known, query_ids, shift, begin, end, top):
        own = jnp.broadcast_to(query_ids.astype(jnp.float32), (rows, rows)).T
        for level in range(begin, end):
            for place, (lv, r) in enumerate(blocks_of(level, top)):
                gap = gap_of(lv, r)
                limit = jnp.where(me >= gap, WINDOW, 0)
                distance = (gap + shift) * rows + row - col
                other = jnp.broadcast_to(ids_buf[known, lv, r].astype(jnp.float32), (rows, rows))
                allowed = (own == other) & (distance >= 0) & (distance < limit)
                table[level, :, place * rows:(place + 1) * rows] = jnp.where(allowed, 0.0, NEG_BIG)

    def make_bias():
        for level in range(top_level - 1):
            wait_diagonal(level, NEAR_IDS)
        fill(bias, 0, ids_buf[0, 0, 0], 0, 0, 1, top_level)

    def make_bias_far():
        for level in range(SERVED in DETOURED, top_level):
            wait_diagonal(level, FAR_IDS)
        fill(bias, 1, ids_buf[0, 0, 0], 0, 1, top_level, top_level)

    def make_bias_up():
        @pl.when(up_ok)
        def _():
            ids_down.wait_recv()
            fill(bias_up, 0, ids_up[...], SPAN, 0, top_level - 1, top_level - 1)

    def stack(wide):
        return jnp.concatenate([wide[:, g * DH:(g + 1) * DH] for g in range(GROUP)], axis=0)

    def unstack(tall):
        return jnp.concatenate([tall[g * rows:(g + 1) * rows] for g in range(GROUP)], axis=1)

    def attend(q, c, level, top, table, state):
        blocks = blocks_of(level, top)
        span = len(blocks) * rows

        def side_of(k):
            main = buf[level, c, :, k].reshape(SPAN * rows, DH)
            if len(blocks) == SPAN:
                return main
            return jnp.concatenate([main, buf[level + 1, c, 0, k]], axis=0)

        t = lax.dot_general(q, side_of(0), (((1,), (1,)), ((), ())), preferred_element_type=jnp.float32)
        t = (t * SCALE2).reshape(GROUP, rows, span) + table[level, :, :span][None]
        t = t.reshape(group_rows, span)
        new = jnp.max(t, axis=1, keepdims=True)
        if state is None:
            new = jnp.broadcast_to(new, (group_rows, DH))
        else:
            new = jnp.maximum(state[0], new)
        p = [jnp.exp2(t[:, r * rows:(r + 1) * rows] - new) for r in range(len(blocks))]
        w = jnp.concatenate([one.astype(jnp.bfloat16) for one in p], axis=1)
        paired = jnp.concatenate([side_of(1), jnp.ones((span, DH), jnp.bfloat16)], axis=1)
        both = jnp.dot(w, paired, preferred_element_type=jnp.float32)
        acc, total = both[:, :DH], both[:, DH:]
        if state is not None:
            fix = jnp.exp2(state[0] - new)
            total = total + state[1] * fix
            acc = acc + state[2] * fix
        return new, total, acc

    def keep(c, state):
        run_max[c], run_sum[c], run_acc[c] = state

    def kept(c):
        return run_max[c], run_sum[c], run_acc[c]

    def query(c):
        return stack(q_buf[:, c * WIDE:(c + 1) * WIDE])

    def finish(c, o):
        out_ref[:, c * WIDE:(c + 1) * WIDE] = unstack(o.astype(out_ref.dtype))

    def near(c):
        if c >= SERVED and c not in DETOURED:
            wait_diagonal(0, c)
        keep(c, attend(query(c), c, 0, top_level, bias, None))

    def far(c):
        for level in range(1, top_level):
            wait_diagonal(level, c)
            state = attend(query(c), c, level, top_level, bias, kept(c))
            if level < top_level - 1:
                keep(c, state)
        _, total, acc = state
        finish(c, acc / total)

    def serve(c):
        for level in range(top_level - 1):
            wait_diagonal(level, c)

        @pl.when(up_ok)
        def _():
            q_down(c).wait_recv()
            state = None
            for level in range(top_level - 1):
                state = attend(stack(q_up[c]), c, level, top_level - 1, bias_up, state)
            most, total, acc = state
            part_out[c] = unstack((acc / total).astype(part_out.dtype))
            lse = most + jnp.log2(total)
            lse_out[c] = jnp.concatenate(
                [
                    jnp.sum(jnp.where(row == col, lse[g * rows:(g + 1) * rows], 0.0), axis=0, keepdims=True)
                    for g in range(GROUP)
                ],
                axis=0,
            )

    def reply(c):
        @pl.when(up_ok)
        def _():
            for one in part_up(c):
                one.start()

    def merge(c):
        @pl.when(down_ok)
        def _():
            for one in part_up(c):
                one.wait_recv()
        most, total, acc = kept(c)
        other = jnp.concatenate(
            [
                jnp.sum(jnp.where(row == col, lse_in[c, g:g + 1, :], 0.0), axis=1, keepdims=True)
                for g in range(GROUP)
            ],
            axis=0,
        )
        new = jnp.maximum(most, other)
        fix, weight = jnp.exp2(most - new), jnp.exp2(other - new)
        o = acc * fix + stack(part_in[c]).astype(jnp.float32) * weight
        finish(c, o / (total * fix + weight))

    def side_x(s, c):
        for k in load(c):
            start(x_copy(s, k))

    def side_y(s, c):
        for k in load(c):
            start(y_copy(s, k))

    def relay(r, one, s, c):
        for k in load(c):
            @pl.when(need(s, spot, spots[r], k))
            def _():
                wait_slot(s - later(spots[r], spot), r, k)
            start(one(s, k))

    actions = (
        arrive, side_x, side_y, functools.partial(relay, 1, relay_x), functools.partial(relay, 2, relay_y),
        lambda s, c: ask(), lambda s, c: clear(), lambda s, c: make_bias(), lambda s, c: make_bias_up(),
        lambda s, c: near(c), lambda s, c: serve(c), lambda s, c: reply(c), lambda s, c: merge(c), lambda s, c: far(c),
        lambda s, c: make_bias_far(), lambda s, c: pass_on(c),
    )
    def settle():
        for c in range(HK + 2):
            for s in range(last_of(c) + 1):
                for cond, one in sends(s, c):
                    pl.when(cond)(one.wait_send)

        @pl.when(down_ok)
        def _():
            ids_down.wait_send()
            for i in range(SERVED):
                q_down(i).wait_send()

        @pl.when(up_ok)
        def _():
            for i in range(SERVED):
                for one in part_up(i):
                    one.wait_send()

    order = ORDER if top_level == 2 else plain_order(top_level)
    for place, code in enumerate(order):
        if place == len(order) - 1:
            settle()
        actions[code // 100](code // 10 % 10, code % 10)


def solution(mesh):
    n = mesh.shape["seq"]

    def local(queries, keys_values, segment_ids):
        rows = queries.shape[0]
        reach = min(WINDOW, n * rows // 2)
        back = -(-(reach - 1) // rows)
        assert n % SPAN == 0 and back % SPAN == 0 and back >= 2 * SPAN
        levels = back // SPAN
        group_rows = GROUP * rows
        return pl.pallas_call(
            functools.partial(kernel, n, rows, back),
            out_shape=pltpu.MemorySpace.VMEM(queries.shape, queries.dtype),
            in_specs=[pl.BlockSpec(memory_space=pl.ANY)] * 3,
            out_specs=pl.BlockSpec(memory_space=pltpu.VMEM),
            scratch_shapes=[
                pltpu.VMEM((levels + 1, HK, SPAN, 2, rows, DH), jnp.bfloat16),
                pltpu.VMEM((2, levels + 1, SPAN, 1, rows), jnp.int32),
                pltpu.VMEM((rows, HQ * DH), jnp.bfloat16),
                pltpu.VMEM((SERVED, rows, WIDE), jnp.bfloat16),
                pltpu.VMEM((1, rows), jnp.int32),
                pltpu.VMEM((SERVED, rows, WIDE), jnp.bfloat16),
                pltpu.VMEM((SERVED, rows, WIDE), jnp.bfloat16),
                pltpu.VMEM((SERVED, GROUP, rows), jnp.float32),
                pltpu.VMEM((SERVED, GROUP, rows), jnp.float32),
                pltpu.VMEM((levels, rows, (SPAN + 1) * rows), jnp.float32),
                pltpu.VMEM((levels - 1, rows, (SPAN + 1) * rows), jnp.float32),
                pltpu.VMEM((HK, group_rows, DH), jnp.float32),
                pltpu.VMEM((HK, group_rows, DH), jnp.float32),
                pltpu.VMEM((HK, group_rows, DH), jnp.float32),
                pltpu.SemaphoreType.DMA((HK + 3,)),
                pltpu.SemaphoreType.DMA((levels + 1, 6, HK + 2)),
                pltpu.SemaphoreType.DMA((levels + 1, SPAN, HK + 2)),
                pltpu.SemaphoreType.DMA((SERVED + 1,)),
                pltpu.SemaphoreType.DMA((SERVED + 1,)),
                pltpu.SemaphoreType.DMA((2, SERVED)),
                pltpu.SemaphoreType.DMA((2, SERVED)),
            ],
            compiler_params=pltpu.CompilerParams(
                collective_id=0, has_side_effects=True, vmem_limit_bytes=60 * 1024 * 1024
            ),
        )(queries, keys_values, segment_ids.reshape(1, rows))

    return jax.shard_map(
        local,
        mesh=mesh,
        in_specs=(P(("rep", "seq"), None), P(None, ("rep", "seq"), None), P(("rep", "seq"))),
        out_specs=P(("rep", "seq"), None),
        check_vma=False,
    )
```
